32 devices in a mesh: groups: 2 (over y), tiles: 8 (over z, x), subwin: 2 (over core).
Axes of the slice: x: 2, y: 2, z: 4, core: 2. Of those that a mesh axis runs over, the one named last changes fastest.
Arguments:
- increment: float32 [64, 8, 16, 16], P(('groups', 'tiles'), 'subwin'), parts along dimension 0, may hold values from -6 to 6
- dual_vector: float32 [64, 8, 16, 16], P(('groups', 'tiles'), 'subwin'), parts along dimension 0, may hold values from -6 to 6
- wind_u: float32 [32, 16, 16], P('tiles'), may hold values from -0.3 to 0.3
- wind_v: float32 [32, 16, 16], P('tiles'), may hold values from -0.3 to 0.3
- land_sea: int32 [32, 16], P('tiles'), may hold values from 0 to 1
- length_sq: float32 [8, 16], P('subwin', 'tiles'), may hold values from 1 to 300
- spread: float32 [8, 16], P('subwin'), may hold values from 0.5 to 3
Outputs:
- model_side: float32 [64, 8, 16, 16], P(('groups', 'tiles'), 'subwin'), parts along dimension 0
- dual_side: float32 [64, 8, 16, 16], P(('groups', 'tiles'), 'subwin'), parts along dimension 0
The draws below stay inside these ranges and needn't reach their ends.
There are 2 independent parts, one for each index of `groups`. The reference program is written for one: setup_inputs(seed, part) draws one part's arguments, and reference() takes and returns one part's arrays. A program takes and returns all parts, laid end to end along the dimension named above; an argument that names none is the same for every part. Nothing has to cross between parts.
All inputs are finite; a program needn't handle non-finite values.
Results may differ from the reference program's by a relative error of at most 0.000098.
Values sent between devices are 32-bit elements; how exact they have to be, the bound alone decides.
No kernel may reach another device: no remote copies, remote signals or barrier semaphores. Data moves between devices by JAX's collectives and lax.ppermute only.
A program may use at most 192 MiB of HBM per device.

```python
import math
import jax
import jax.numpy as jnp
from jax import lax

LEV = 16
STEPS = 8
SWEEPS = 4
SUBWINS = 8
NLON = 32
NLAT = 16


def draw_wind_u(key, part):
    keys = jax.random.split(jax.random.fold_in(key, 23), 2)
    direction = (2 * jax.random.randint(keys[0], (1, LEV, NLAT), 0, 2) - 1).astype(jnp.float32)
    magnitude = jax.random.uniform(keys[1], (NLON, LEV, NLAT), jnp.float32, 0.15, 0.3)
    return direction * magnitude


def draw_land_sea(key, part):
    keys = jax.random.split(jax.random.fold_in(key, 11), 3)
    period = jax.random.randint(keys[0], (NLAT,), 24, 64)
    width = jax.random.randint(keys[1], (NLAT,), 12, 20)
    offset = jax.random.randint(keys[2], (NLAT,), 0, 64)
    index = jnp.arange(NLON, dtype=jnp.int32)[:, None]
    return ((index + offset[None, :]) % period[None, :] < width[None, :]).astype(jnp.int32)


def shard_levels(own_key, dims, shards, smallest, high):
    level = 1.0
    for axis_at, blocks in shards:
        draws = jax.random.uniform(jax.random.fold_in(jax.random.fold_in(own_key, 6), axis_at), (blocks,), jnp.float32, smallest / len(shards), high / len(shards))
        level = level * jnp.repeat(jnp.exp(draws), dims[axis_at] // blocks).reshape((-1,) + (1,) * (len(dims) - 1 - axis_at))
    return level


def noise(rng, shape, scale, bound, shards=(), kind=jnp.bfloat16):
    loudness = shard_levels(rng, shape, shards, -0.22, 0.18) if shards else 1.0
    values = jax.random.normal(rng, shape, jnp.float32) * scale * loudness
    return jnp.minimum(jnp.maximum(values, -bound), bound).astype(kind)


def setup_inputs(seed: int = 0, part: int = 0) -> dict:
    key_of = jax.random.split(jax.random.key(seed), 8)
    own_keys = jax.random.split(jax.random.fold_in(key_of[7], part), 8)
    return {
        "increment": noise(own_keys[0], (NLON, SUBWINS, LEV, NLAT), 1.0, 6.0, ((0, 8), (1, 2)), jnp.float32),
        "dual_vector": noise(own_keys[1], (NLON, SUBWINS, LEV, NLAT), 1.0, 6.0, ((0, 8), (1, 2)), jnp.float32),
        "wind_u": draw_wind_u(jax.random.fold_in(key_of[7], 71), part),
        "wind_v": jnp.clip(jax.random.uniform(key_of[3], (NLON, LEV, NLAT), jnp.float32, -0.3, 0.3) * shard_levels(key_of[3], (NLON, LEV, NLAT), ((0, 8),), -0.4, 0.0), -0.3, 0.3),
        "land_sea": draw_land_sea(jax.random.fold_in(key_of[7], 71), part),
        "length_sq": jnp.clip(jnp.exp(math.log(300.0) - 5.7037825 * jax.random.uniform(key_of[5], (SUBWINS, NLAT), jnp.float32) ** shard_levels(key_of[5], (SUBWINS, NLAT), ((0, 2), (1, 8)), -0.2, 0.2)), 1.0, 300.0),
        "spread": jnp.clip(jnp.exp(math.log(3.0) - 1.7917595 * jax.random.uniform(key_of[6], (SUBWINS, LEV), jnp.float32) ** shard_levels(key_of[6], (SUBWINS, LEV), ((0, 2),), -0.2, 0.2)), 0.5, 3.0),
    }


def from_north(values):
    return jnp.concatenate([values[..., 1:], jnp.zeros_like(values[..., :1])], axis=-1)


def from_south(values):
    return jnp.concatenate([jnp.zeros_like(values[..., :1]), values[..., :-1]], axis=-1)


def coefficients(wind_u, wind_v, land_sea):
    mixing = (0.15 + 0.09 * land_sea.astype(jnp.float32))[:, None, :]
    return (1.0 - 4.0 * mixing, mixing - 0.5 * wind_u, mixing + 0.5 * wind_u, mixing - 0.5 * wind_v, mixing + 0.5 * wind_v)


def tangent_model(fields, coeffs):
    centre, eastward, westward, northward, southward = coeffs
    for repeat in range(STEPS):
        fields = (centre * fields + eastward * jnp.roll(fields, -1, 0) + westward * jnp.roll(fields, 1, 0)
                  + northward * from_north(fields) + southward * from_south(fields))
    return fields


def adjoint_model(fields, coeffs):
    centre, eastward, westward, northward, southward = coeffs
    for repeat in range(STEPS):
        fields = (centre * fields + jnp.roll(eastward * fields, 1, 0) + jnp.roll(westward * fields, -1, 0)
                  + from_south(northward * fields) + from_north(southward * fields))
    return fields


def smooth_one(pair):
    weighted, lengths = pair
    spectra = jnp.fft.rfft(weighted, axis=0)
    wave = jnp.arange(NLON // 2 + 1).astype(jnp.float32)
    basic = 1.0 - jnp.cos(wave * (2.0 * math.pi / NLON))
    damping = (1.0 + 2.0 * lengths[None, None, :] * basic[:, None, None]) ** (-SWEEPS)
    return jnp.fft.irfft(spectra * damping, n=NLON, axis=0).astype(weighted.dtype)


def reference(increment, dual_vector, wind_u, wind_v, land_sea, length_sq, spread):
    coeffs = coefficients(wind_u, wind_v, land_sea)
    previous = jnp.concatenate([jnp.zeros_like(increment[:, :1]), increment[:, :-1]], axis=1)
    following = jnp.concatenate([dual_vector[:, 1:], jnp.zeros_like(dual_vector[:, :1])], axis=1)
    forward = lax.map(lambda fields: tangent_model(fields, coeffs), jnp.moveaxis(previous, 1, 0))
    forward = jnp.moveaxis(forward, 0, 1)
    backward = lax.map(lambda fields: adjoint_model(fields, coeffs), jnp.moveaxis(following, 1, 0))
    backward = jnp.moveaxis(backward, 0, 1)
    weighted = dual_vector * spread[None, :, :, None]
    smoothed = lax.map(smooth_one, (jnp.moveaxis(weighted, 1, 0), length_sq))
    covar = jnp.moveaxis(smoothed, 0, 1) * spread[None, :, :, None]
    return covar + increment - forward, dual_vector - backward
```

```python
import functools
import math

import jax
import jax.numpy as jnp
from jax import lax
from jax.experimental import pallas as pl
from jax.experimental.pallas import tpu as pltpu
from jax.sharding import PartitionSpec as P

STEPS = 8
SWEEPS = 4
LON_DEV = 4


def extended(x, sides, width):
    for axis, dim in sides:
        devices, length = (lax.axis_size(axis), x.shape[dim])
        up = [(i, (i + 1) % devices) for i in range(devices)]
        down = [(j, i) for i, j in up]
        last = lax.slice_in_dim(x, length - width, length, axis=dim)
        leading = lax.slice_in_dim(x, 0, width, axis=dim)
        before = lax.ppermute(last, axis, up)
        after = lax.ppermute(leading, axis, down)
        x = jnp.concatenate([before, x, after], axis=dim)
    return x


def passed_along(x, axis, by):
    devices = lax.axis_size(axis)
    pairs = [(i, i + by) for i in range(devices) if 0 <= i + by < devices]
    return lax.ppermute(x, axis, pairs)


def from_north(values):
    return jnp.concatenate([values[..., 1:], jnp.zeros_like(values[..., :1])], axis=-1)


def from_south(values):
    return jnp.concatenate([jnp.zeros_like(values[..., :1]), values[..., :-1]], axis=-1)


def coefficients(wind_u, wind_v, mixing):
    return (
        1.0 - 4.0 * mixing,
        mixing - 0.5 * wind_u,
        mixing + 0.5 * wind_u,
        mixing - 0.5 * wind_v,
        mixing + 0.5 * wind_v,
    )


def tangent_step(fields, coeffs, offset):
    extent = fields.shape[0]
    centre, eastward, westward, northward, southward = [
        coeff[offset + 1 : offset + extent - 1][:, None] for coeff in coeffs
    ]
    middle = fields[1:-1]
    return (
        centre * middle
        + eastward * fields[2:]
        + westward * fields[:-2]
        + northward * from_north(middle)
        + southward * from_south(middle)
    )


def adjoint_step(fields, coeffs, offset):
    extent = fields.shape[0]
    centre = coeffs[0][offset + 1 : offset + extent - 1][:, None]
    northward = coeffs[3][offset + 1 : offset + extent - 1][:, None]
    southward = coeffs[4][offset + 1 : offset + extent - 1][:, None]
    eastward = coeffs[1][offset : offset + extent][:, None]
    westward = coeffs[2][offset : offset + extent][:, None]
    middle = fields[1:-1]
    return (
        centre * middle
        + (eastward * fields)[:-2]
        + (westward * fields)[2:]
        + from_south(northward * middle)
        + from_north(southward * middle)
    )


def run_tangent(fields, coeffs, margin):
    for repeat in range(STEPS // margin):
        grown = extended(fields, (("tiles", 0),), margin)
        for inner_step in range(margin):
            offset = (coeffs[0].shape[0] - grown.shape[0]) // 2
            grown = tangent_step(grown, coeffs, offset)
        fields = grown
    return fields


def run_adjoint(fields, coeffs, margin):
    for repeat in range(STEPS // margin):
        grown = extended(fields, (("tiles", 0),), margin)
        for inner_step in range(margin):
            offset = (coeffs[0].shape[0] - grown.shape[0]) // 2
            grown = adjoint_step(grown, coeffs, offset)
        fields = grown
    return fields


def square_tables(extent):
    index = jnp.arange(extent, dtype=jnp.int32)
    phases = index[:, None] * index[None, :] % extent
    angles = phases.astype(jnp.float32) * (2.0 * math.pi / extent)
    return (jnp.cos(angles), jnp.sin(angles))


def contract(form, first, second):
    return jnp.einsum(form, first, second, precision=lax.Precision.HIGHEST)


def smooth_bands(bands, length_sq):
    count = bands.shape[0]
    inner = LON_DEV
    outer = count // inner
    columns = bands.reshape(outer, inner, -1)
    cos_outer, sin_outer = square_tables(outer)
    cos_inner, sin_inner = square_tables(inner)
    outer_index = jnp.arange(outer, dtype=jnp.int32)
    inner_index = jnp.arange(inner, dtype=jnp.int32)
    twist = (outer_index[:, None] * inner_index[None, :] % count).astype(jnp.float32) * (
        2.0 * math.pi / count
    )
    twist_cos = jnp.cos(twist)[:, :, None]
    twist_sin = jnp.sin(twist)[:, :, None]
    first_real = contract("ab,bqc->aqc", cos_outer, columns)
    first_imag = -contract("ab,bqc->aqc", sin_outer, columns)
    turned_real = first_real * twist_cos + first_imag * twist_sin
    turned_imag = first_imag * twist_cos - first_real * twist_sin
    modes_real = contract("aqc,kq->akc", turned_real, cos_inner) + contract(
        "aqc,kq->akc", turned_imag, sin_inner
    )
    modes_imag = contract("aqc,kq->akc", turned_imag, cos_inner) - contract(
        "aqc,kq->akc", turned_real, sin_inner
    )
    wave = (outer_index[:, None] + outer * inner_index[None, :]).astype(jnp.float32)
    basic = 1.0 - jnp.cos(wave * (2.0 * math.pi / count))
    damping = (1.0 + 2.0 * length_sq[None, None, :, None, :] * basic[:, :, None, None, None]) ** (
        -SWEEPS
    )
    damping = jnp.broadcast_to(damping, (outer, inner) + bands.shape[1:]).reshape(outer, inner, -1)
    modes_real = modes_real * damping
    modes_imag = modes_imag * damping
    back_real = contract("akc,kq->aqc", modes_real, cos_inner) - contract(
        "akc,kq->aqc", modes_imag, sin_inner
    )
    back_imag = contract("akc,kq->aqc", modes_imag, cos_inner) + contract(
        "akc,kq->aqc", modes_real, sin_inner
    )
    final_real = back_real * twist_cos - back_imag * twist_sin
    final_imag = back_imag * twist_cos + back_real * twist_sin
    smoothed = contract("ab,bqc->aqc", cos_outer, final_real) - contract(
        "ab,bqc->aqc", sin_outer, final_imag
    )
    return (smoothed / count).reshape(bands.shape)


def body(increment, dual_vector, wind_u, wind_v, land_sea, length_sq, spread):
    margin = 4
    mixing = 0.15 + 0.09 * land_sea.astype(jnp.float32)
    grown_u, grown_v, grown_mix = (
        extended(wind_u, (("tiles", 0),), margin),
        extended(wind_v, (("tiles", 0),), margin),
        extended(mixing, (("tiles", 0),), margin),
    )
    coeffs = coefficients(grown_u, grown_v, grown_mix[:, None, :])
    carried = passed_along(increment[:, -1:], "subwin", 1)
    previous = jnp.concatenate([carried, increment[:, :-1]], axis=1)
    later = passed_along(dual_vector[:, :1], "subwin", -1)
    following = jnp.concatenate([dual_vector[:, 1:], later], axis=1)
    weighted = dual_vector * spread[None, :, :, None]
    bands = lax.all_to_all(weighted, "tiles", split_axis=3, concat_axis=0, tiled=True)
    smoothed = smooth_bands(bands, length_sq)
    forward = run_tangent(previous, coeffs, margin)
    backward = run_adjoint(following, coeffs, margin)
    returned = lax.all_to_all(smoothed, "tiles", split_axis=0, concat_axis=3, tiled=True)
    covar = returned * spread[None, :, :, None]
    return (covar + increment - forward, dual_vector - backward)


SUB = 8
LANES = 128


def dense_fits(mesh, shape, lats):
    lons, wins, levels, _ = shape
    tiles = mesh.shape["tiles"]
    halves = levels // SUB
    return (
        levels % SUB == 0
        and wins * halves * lats == LANES
        and lons * halves * lats == LANES
        and lats % tiles == 0
        and lons * lats + wins * (lats // tiles) <= LANES
        and mesh.shape["subwin"] == 2
        and tiles % 2 == 0
        and tiles // 2 >= 3
        and STEPS <= 2 * lons
    )


def lane_index():
    return lax.broadcasted_iota(jnp.int32, (SUB, LANES), 1)


def picked(values, index):
    return jnp.take_along_axis(values, index, axis=1)


def pack_kernel(inc_ref, dual_ref, u_ref, v_ref, land_ref, len_ref, main_ref, extra_ref):
    lons, wins, levels, lats = inc_ref.shape
    halves = levels // SUB
    own_lats = len_ref.shape[1]
    lane = lane_index()
    first = lax.axis_index("subwin") == 0

    def put(ref, row, slot, value):
        ref[row * SUB : (row + 1) * SUB, slot * lats : (slot + 1) * lats] = value

    for i in range(lons):
        for half in range(halves):
            rows = slice(half * SUB, (half + 1) * SUB)
            for s in range(wins):
                put(main_ref, i, s * halves + half, dual_ref[i, s, rows, :])
                put(main_ref, lons + i, s * halves + half, inc_ref[i, s, rows, :])
            put(main_ref, 2 * lons, i * halves + half, u_ref[i, rows, :])
            put(main_ref, 2 * lons + 1, i * halves + half, v_ref[i, rows, :])
            edge = jnp.where(first, inc_ref[i, wins - 1, rows, :], dual_ref[i, 0, rows, :])
            put(extra_ref, 0, i * halves + half, edge)
    base = (2 * lons + 2) * SUB
    main_ref[base : base + SUB, :] = jnp.zeros((SUB, LANES), jnp.float32)
    for i in range(lons):
        mixing = 0.15 + 0.09 * land_ref[i : i + 1, :].astype(jnp.float32)
        main_ref[base : base + SUB, i * lats : (i + 1) * lats] = jnp.broadcast_to(mixing, (SUB, lats))
    for s in range(wins):
        at = lons * lats + s * own_lats
        main_ref[base : base + SUB, at : at + own_lats] = jnp.broadcast_to(
            len_ref[s : s + 1, :], (SUB, own_lats)
        )


def apply_kernel(geometry, *refs):
    lons, wins, levels, lats, tiles = geometry
    halves = levels // SUB
    group = halves * lats
    rings = tiles // 2
    own_lats = lats // tiles
    count = lons * tiles
    main_ref, extra_ref, pmain_ref, pextra_ref, left_ref, right_ref = refs[:6]
    far_refs = refs[6 : 6 + rings - 3]
    spread_ref, model_ref, dual_out_ref, coeff_ref, field_ref, dual_ref = refs[6 + rings - 3 :]
    lane = lane_index()
    tile = lax.axis_index("tiles")
    even = tile % 2 == 0
    first = lax.axis_index("subwin") == 0
    main_rows = (2 * lons + 3) * SUB
    block_rows = main_rows + SUB
    far_rows = (lons + 1) * SUB

    def block(ring, peer, row):
        ring = (ring + rings // 2 - 1) % rings - (rings // 2 - 1)
        if ring == 0:
            if row == 2 * lons + 3:
                ref, at = (pextra_ref if peer else extra_ref), 0
            else:
                ref, at = (pmain_ref if peer else main_ref), row * SUB
        elif ring in (-1, 1):
            ref, at = (right_ref if ring == 1 else left_ref), row * SUB + (block_rows if peer else 0)
        else:
            if row >= lons:
                row = lons
            ref, at = far_refs[ring % rings - 2], row * SUB + (far_rows if peer else 0)
        return ref[at : at + SUB, :]

    def at_tile(offset, row):
        if offset % 2 == 0:
            return block(offset // 2, False, row)
        return jnp.where(even, block((offset - 1) // 2, True, row), block((offset + 1) // 2, True, row))

    misc_row = 2 * lons + 2

    length = jnp.zeros((SUB, LANES), jnp.float32)
    index = lons * lats + own_lats * (lane // group) + lane % own_lats
    owner = lane % lats // own_lats
    low = -(tiles // 2) + 1
    for offset in range(low, low + tiles):
        here = picked(at_tile(offset, misc_row), index)
        length = jnp.where(owner == (tile + offset + tiles) % tiles, here, length)
    damped = []
    for wave in range(count // 2 + 1):
        basic = 1.0 - math.cos(2.0 * math.pi * wave / count)
        inverse = 1.0 / (1.0 + (2.0 * basic) * length)
        squared = inverse * inverse
        weight = (1.0 if wave in (0, count // 2) else 2.0) / count
        damped.append(squared * squared * weight)
    weights = []
    for gap in range(count // 2 + 1):
        total = None
        for wave in range(count // 2 + 1):
            term = damped[wave] * math.cos(2.0 * math.pi * (wave * gap % count) / count)
            total = term if total is None else total + term
        weights.append(total)

    smooth = [None] * lons
    for offset in range(low, low + tiles):
        for j in range(lons):
            value = at_tile(offset, j)
            for i in range(lons):
                gap = (i - (offset * lons + j)) % count
                term = weights[min(gap, count - gap)] * value
                smooth[i] = term if smooth[i] is None else smooth[i] + term

    lat = lane % lats
    span = lons + 2 * STEPS
    for r in range(span):
        offset, i = (r - STEPS) // lons, (r - STEPS) % lons
        spot = i * group + lane % group
        wind_u = 0.5 * picked(at_tile(offset, 2 * lons), spot)
        wind_v = 0.5 * picked(at_tile(offset, 2 * lons + 1), spot)
        mixing = picked(at_tile(offset, misc_row), i * lats + lat)
        coeff_ref[r, 0] = 1.0 - 4.0 * mixing
        coeff_ref[r, 1] = mixing - wind_u
        coeff_ref[r, 2] = mixing + wind_u
        coeff_ref[r, 3] = jnp.where(lat == lats - 1, 0.0, mixing - wind_v)
        coeff_ref[r, 4] = jnp.where(lat == 0, 0.0, mixing + wind_v)
        edge = at_tile(offset, 2 * lons + 3)
        early = pltpu.roll(edge, (LANES - i * group) % LANES, 1)
        late = pltpu.roll(edge, (2 * LANES - (i + 1) * group) % LANES, 1)
        inside = pltpu.roll(at_tile(offset, lons + i), group, 1)
        field_ref[r] = jnp.where(lane < group, jnp.where(first, 0.0, early), inside)
        inside = pltpu.roll(at_tile(offset, i), LANES - group, 1)
        dual_ref[r] = jnp.where(lane >= LANES - group, jnp.where(first, late, 0.0), inside)

    def north(values):
        return pltpu.roll(values, LANES - 1, 1)

    def south(values):
        return pltpu.roll(values, 1, 1)

    forward = [field_ref[r] for r in range(span)]
    for step in range(STEPS):
        following = []
        for p in range(1, len(forward) - 1):
            r = p + step
            middle = forward[p]
            following.append(
                coeff_ref[r, 0] * middle
                + coeff_ref[r, 1] * forward[p + 1]
                + coeff_ref[r, 2] * forward[p - 1]
                + coeff_ref[r, 3] * north(middle)
                + coeff_ref[r, 4] * south(middle)
            )
        forward = following
    backward = [dual_ref[r] for r in range(span)]
    for step in range(STEPS):
        following = []
        for p in range(1, len(backward) - 1):
            r = p + step
            middle = backward[p]
            following.append(
                coeff_ref[r, 0] * middle
                + coeff_ref[r - 1, 1] * backward[p - 1]
                + coeff_ref[r + 1, 2] * backward[p + 1]
                + south(coeff_ref[r, 3] * middle)
                + north(coeff_ref[r, 4] * middle)
            )
        backward = following

    level = lax.broadcasted_iota(jnp.int32, (SUB, LANES), 0) + SUB * (lane % group // lats)
    scale = jnp.zeros((SUB, LANES), jnp.float32)
    for s in range(wins):
        row = jnp.concatenate(
            [jnp.broadcast_to(spread_ref[s : s + 1, :], (SUB, levels))] * (LANES // levels), axis=1
        )
        scale = jnp.where(lane // group == s, picked(row, level), scale)
    square = scale * scale

    for i in range(lons):
        model = square * smooth[i] + block(0, False, lons + i) - forward[i]
        other = block(0, False, i) - backward[i]
        for s in range(wins):
            for half in range(halves):
                at = (s * halves + half) * lats
                rows = slice(half * SUB, (half + 1) * SUB)
                model_ref[i, s, rows, :] = model[:, at : at + lats]
                dual_out_ref[i, s, rows, :] = other[:, at : at + lats]


def dense_body(increment, dual_vector, wind_u, wind_v, land_sea, length_sq, spread):
    lons, wins, levels, lats = increment.shape
    tiles = lax.axis_size("tiles")
    cores = lax.axis_size("subwin")
    rings = tiles // 2
    main_rows = (2 * lons + 3) * SUB
    vmem = pl.BlockSpec(memory_space=pltpu.VMEM)
    main, extra = pl.pallas_call(
        pack_kernel,
        out_shape=(
            jax.ShapeDtypeStruct((main_rows, LANES), jnp.float32),
            jax.ShapeDtypeStruct((SUB, LANES), jnp.float32),
        ),
        in_specs=[vmem] * 6,
        out_specs=(vmem, vmem),
        name="pack",
    )(increment, dual_vector, wind_u, wind_v, land_sea, length_sq)

    other = [(w, cores - 1 - w) for w in range(cores)]
    peer = [(t, t ^ 1) for t in range(tiles)]
    across = [
        (t * cores + w, (t ^ 1) * cores + cores - 1 - w) for t in range(tiles) for w in range(cores)
    ]
    swapped = lax.ppermute(extra, "subwin", other)
    peer_main = lax.ppermute(main, "tiles", peer)
    peer_extra = lax.ppermute(extra, ("tiles", "subwin"), across)

    def ring(x, by):
        return lax.ppermute(
            x, "tiles", [(t, (t // 2 + by) % rings * 2 + t % 2) for t in range(tiles)]
        )

    pair = jnp.concatenate([main, swapped, peer_main, peer_extra])
    held, misc = lons * SUB, (2 * lons + 2) * SUB
    short = jnp.concatenate(
        [main[:held], main[misc:], peer_main[:held], peer_main[misc:]]
    )
    left = ring(pair, 1)
    right = ring(pair, -1)
    far = [ring(short, -d) for d in range(2, rings - 1)]
    span = lons + 2 * STEPS
    shape = jax.ShapeDtypeStruct(increment.shape, jnp.float32)
    inputs = [main, swapped, peer_main, peer_extra, left, right, *far, spread]
    return pl.pallas_call(
        functools.partial(apply_kernel, (lons, wins, levels, lats, tiles)),
        out_shape=(shape, shape),
        in_specs=[vmem] * len(inputs),
        out_specs=(vmem, vmem),
        scratch_shapes=[
            pltpu.VMEM((span, 5, SUB, LANES), jnp.float32),
            pltpu.VMEM((span, SUB, LANES), jnp.float32),
            pltpu.VMEM((span, SUB, LANES), jnp.float32),
        ],
        name="apply",
    )(*inputs)


def solution(mesh):
    placed = (
        P(("groups", "tiles"), "subwin", None, None),
        P(("groups", "tiles"), "subwin", None, None),
        P("tiles", None, None),
        P("tiles", None, None),
        P("tiles", None),
        P("subwin", "tiles"),
        P("subwin", None),
    )

    def local(*arrays):
        increment = arrays[0]
        lats = increment.shape[3]
        chosen = dense_body if dense_fits(mesh, increment.shape, lats) else body
        return chosen(*arrays)

    return jax.shard_map(
        local,
        mesh=mesh,
        in_specs=placed,
        out_specs=(
            P(("groups", "tiles"), "subwin", None, None),
            P(("groups", "tiles"), "subwin", None, None),
        ),
        check_vma=False,
    )
```

```python
import functools
import math

import jax
import jax.numpy as jnp
from jax import lax
from jax.experimental import pallas as pl
from jax.experimental.pallas import tpu as pltpu
from jax.sharding import PartitionSpec as P

STEPS = 8
SWEEPS = 4
LON_DEV = 4


def extended(x, sides, width):
    for axis, dim in sides:
        devices, length = (lax.axis_size(axis), x.shape[dim])
        up = [(i, (i + 1) % devices) for i in range(devices)]
        down = [(j, i) for i, j in up]
        last = lax.slice_in_dim(x, length - width, length, axis=dim)
        leading = lax.slice_in_dim(x, 0, width, axis=dim)
        before = lax.ppermute(last, axis, up)
        after = lax.ppermute(leading, axis, down)
        x = jnp.concatenate([before, x, after], axis=dim)
    return x


def passed_along(x, axis, by):
    devices = lax.axis_size(axis)
    pairs = [(i, i + by) for i in range(devices) if 0 <= i + by < devices]
    return lax.ppermute(x, axis, pairs)


def from_north(values):
    return jnp.concatenate([values[..., 1:], jnp.zeros_like(values[..., :1])], axis=-1)


def from_south(values):
    return jnp.concatenate([jnp.zeros_like(values[..., :1]), values[..., :-1]], axis=-1)


def coefficients(wind_u, wind_v, mixing):
    return (
        1.0 - 4.0 * mixing,
        mixing - 0.5 * wind_u,
        mixing + 0.5 * wind_u,
        mixing - 0.5 * wind_v,
        mixing + 0.5 * wind_v,
    )


def tangent_step(fields, coeffs, offset):
    extent = fields.shape[0]
    centre, eastward, westward, northward, southward = [
        coeff[offset + 1 : offset + extent - 1][:, None] for coeff in coeffs
    ]
    middle = fields[1:-1]
    return (
        centre * middle
        + eastward * fields[2:]
        + westward * fields[:-2]
        + northward * from_north(middle)
        + southward * from_south(middle)
    )


def adjoint_step(fields, coeffs, offset):
    extent = fields.shape[0]
    centre = coeffs[0][offset + 1 : offset + extent - 1][:, None]
    northward = coeffs[3][offset + 1 : offset + extent - 1][:, None]
    southward = coeffs[4][offset + 1 : offset + extent - 1][:, None]
    eastward = coeffs[1][offset : offset + extent][:, None]
    westward = coeffs[2][offset : offset + extent][:, None]
    middle = fields[1:-1]
    return (
        centre * middle
        + (eastward * fields)[:-2]
        + (westward * fields)[2:]
        + from_south(northward * middle)
        + from_north(southward * middle)
    )


def run_tangent(fields, coeffs, margin):
    for repeat in range(STEPS // margin):
        grown = extended(fields, (("tiles", 0),), margin)
        for inner_step in range(margin):
            offset = (coeffs[0].shape[0] - grown.shape[0]) // 2
            grown = tangent_step(grown, coeffs, offset)
        fields = grown
    return fields


def run_adjoint(fields, coeffs, margin):
    for repeat in range(STEPS // margin):
        grown = extended(fields, (("tiles", 0),), margin)
        for inner_step in range(margin):
            offset = (coeffs[0].shape[0] - grown.shape[0]) // 2
            grown = adjoint_step(grown, coeffs, offset)
        fields = grown
    return fields


def square_tables(extent):
    index = jnp.arange(extent, dtype=jnp.int32)
    phases = index[:, None] * index[None, :] % extent
    angles = phases.astype(jnp.float32) * (2.0 * math.pi / extent)
    return (jnp.cos(angles), jnp.sin(angles))


def contract(form, first, second):
    return jnp.einsum(form, first, second, precision=lax.Precision.HIGHEST)


def smooth_bands(bands, length_sq):
    count = bands.shape[0]
    inner = LON_DEV
    outer = count // inner
    columns = bands.reshape(outer, inner, -1)
    cos_outer, sin_outer = square_tables(outer)
    cos_inner, sin_inner = square_tables(inner)
    outer_index = jnp.arange(outer, dtype=jnp.int32)
    inner_index = jnp.arange(inner, dtype=jnp.int32)
    twist = (outer_index[:, None] * inner_index[None, :] % count).astype(jnp.float32) * (
        2.0 * math.pi / count
    )
    twist_cos = jnp.cos(twist)[:, :, None]
    twist_sin = jnp.sin(twist)[:, :, None]
    first_real = contract("ab,bqc->aqc", cos_outer, columns)
    first_imag = -contract("ab,bqc->aqc", sin_outer, columns)
    turned_real = first_real * twist_cos + first_imag * twist_sin
    turned_imag = first_imag * twist_cos - first_real * twist_sin
    modes_real = contract("aqc,kq->akc", turned_real, cos_inner) + contract(
        "aqc,kq->akc", turned_imag, sin_inner
    )
    modes_imag = contract("aqc,kq->akc", turned_imag, cos_inner) - contract(
        "aqc,kq->akc", turned_real, sin_inner
    )
    wave = (outer_index[:, None] + outer * inner_index[None, :]).astype(jnp.float32)
    basic = 1.0 - jnp.cos(wave * (2.0 * math.pi / count))
    damping = (1.0 + 2.0 * length_sq[None, None, :, None, :] * basic[:, :, None, None, None]) ** (
        -SWEEPS
    )
    damping = jnp.broadcast_to(damping, (outer, inner) + bands.shape[1:]).reshape(outer, inner, -1)
    modes_real = modes_real * damping
    modes_imag = modes_imag * damping
    back_real = contract("akc,kq->aqc", modes_real, cos_inner) - contract(
        "akc,kq->aqc", modes_imag, sin_inner
    )
    back_imag = contract("akc,kq->aqc", modes_imag, cos_inner) + contract(
        "akc,kq->aqc", modes_real, sin_inner
    )
    final_real = back_real * twist_cos - back_imag * twist_sin
    final_imag = back_imag * twist_cos + back_real * twist_sin
    smoothed = contract("ab,bqc->aqc", cos_outer, final_real) - contract(
        "ab,bqc->aqc", sin_outer, final_imag
    )
    return (smoothed / count).reshape(bands.shape)


def body(increment, dual_vector, wind_u, wind_v, land_sea, length_sq, spread):
    margin = 4
    mixing = 0.15 + 0.09 * land_sea.astype(jnp.float32)
    grown_u, grown_v, grown_mix = (
        extended(wind_u, (("tiles", 0),), margin),
        extended(wind_v, (("tiles", 0),), margin),
        extended(mixing, (("tiles", 0),), margin),
    )
    coeffs = coefficients(grown_u, grown_v, grown_mix[:, None, :])
    carried = passed_along(increment[:, -1:], "subwin", 1)
    previous = jnp.concatenate([carried, increment[:, :-1]], axis=1)
    later = passed_along(dual_vector[:, :1], "subwin", -1)
    following = jnp.concatenate([dual_vector[:, 1:], later], axis=1)
    weighted = dual_vector * spread[None, :, :, None]
    bands = lax.all_to_all(weighted, "tiles", split_axis=3, concat_axis=0, tiled=True)
    smoothed = smooth_bands(bands, length_sq)
    forward = run_tangent(previous, coeffs, margin)
    backward = run_adjoint(following, coeffs, margin)
    returned = lax.all_to_all(smoothed, "tiles", split_axis=0, concat_axis=3, tiled=True)
    covar = returned * spread[None, :, :, None]
    return (covar + increment - forward, dual_vector - backward)


SUB = 8
LANES = 128
VMEM_BYTES = 4 * 2**20


def dense_fits(mesh, shape, lats):
    lons, wins, levels, _ = shape
    tiles = mesh.shape["tiles"]
    halves = levels // SUB
    return (
        levels % SUB == 0
        and wins * halves * lats == LANES
        and lons * halves * lats == LANES
        and lats % tiles == 0
        and lons * lats + wins * (lats // tiles) <= LANES
        and mesh.shape["subwin"] == 2
        and tiles % 2 == 0
        and tiles // 2 >= 4
        and STEPS <= 2 * lons
    )


def lane_index():
    return lax.broadcasted_iota(jnp.int32, (SUB, LANES), 1)


def picked(values, index):
    return jnp.take_along_axis(values, index, axis=1)


def pack_kernel(*refs):
    arrays, (main_ref, extra_ref), held, arrived = refs[:6], refs[6:8], refs[8:14], refs[14]
    copies = [
        pltpu.make_async_copy(source, target, arrived.at[k])
        for k, (source, target) in enumerate(zip(arrays, held))
    ]
    for copy in copies:
        copy.start()
    for copy in copies:
        copy.wait()
    inc_ref, dual_ref, u_ref, v_ref, land_ref, len_ref = held
    lons, wins, levels, lats = inc_ref.shape
    halves = levels // SUB
    own_lats = len_ref.shape[0]
    first = lax.axis_index("subwin") == 0

    def put(ref, row, slot, value):
        ref[row * SUB : (row + 1) * SUB, slot * lats : (slot + 1) * lats] = value

    for i in range(lons):
        for half in range(halves):
            rows = slice(half * SUB, (half + 1) * SUB)
            for s in range(wins):
                put(main_ref, i, s * halves + half, dual_ref[i, s, rows, :])
                put(main_ref, lons + i, s * halves + half, inc_ref[i, s, rows, :])
            put(main_ref, 2 * lons, i * halves + half, u_ref[i, rows, :])
            put(main_ref, 2 * lons + 1, i * halves + half, v_ref[i, rows, :])
            edge = jnp.where(first, inc_ref[i, wins - 1, rows, :], dual_ref[i, 0, rows, :])
            put(extra_ref, 0, i * halves + half, edge)
    base = (2 * lons + 2) * SUB
    main_ref[base : base + SUB, :] = jnp.zeros((SUB, LANES), jnp.float32)
    for i in range(lons):
        mixing = 0.15 + 0.09 * land_ref[i : i + 1, :].astype(jnp.float32)
        main_ref[base : base + SUB, i * lats : (i + 1) * lats] = jnp.broadcast_to(mixing, (SUB, lats))
    for j in range(own_lats):
        at = lons * lats + j * wins
        main_ref[base : base + SUB, at : at + wins] = jnp.broadcast_to(
            len_ref[j : j + 1, :], (SUB, wins)
        )


def apply_kernel(geometry, *refs):
    lons, wins, levels, lats, tiles = geometry
    halves = levels // SUB
    group = halves * lats
    rings = tiles // 2
    own_lats = lats // tiles
    count = lons * tiles
    main_ref, extra_ref, pmain_ref, pextra_ref, left_ref, right_ref = refs[:6]
    far_refs = refs[6 : 6 + rings - 3]
    spread_ref, model_ref, dual_out_ref, coeff_ref, field_ref, dual_ref = refs[6 + rings - 3 :]
    lane = lane_index()
    tile = lax.axis_index("tiles")
    even = tile % 2 == 0
    first = lax.axis_index("subwin") == 0
    main_rows = (2 * lons + 3) * SUB
    block_rows = main_rows + SUB
    far_rows = (lons + 1) * SUB

    def block(ring, peer, row):
        ring = (ring + rings // 2 - 1) % rings - (rings // 2 - 1)
        if ring == 0:
            if row == 2 * lons + 3:
                ref, at = (pextra_ref if peer else extra_ref), 0
            else:
                ref, at = (pmain_ref if peer else main_ref), row * SUB
        elif ring in (-1, 1):
            ref, at = (right_ref if ring == 1 else left_ref), row * SUB + (block_rows if peer else 0)
        else:
            if row >= lons:
                row = lons
            ref, at = far_refs[ring % rings - 2], row * SUB + (far_rows if peer else 0)
        return ref[at : at + SUB, :]

    def at_tile(offset, row):
        if offset % 2 == 0:
            return block(offset // 2, False, row)
        return jnp.where(even, block((offset - 1) // 2, True, row), block((offset + 1) // 2, True, row))

    misc_row = 2 * lons + 2

    length = jnp.zeros((SUB, LANES), jnp.float32)
    index = lons * lats + wins * (lane % own_lats) + lane // group
    owner = lane % lats // own_lats
    low = -(tiles // 2) + 1
    for offset in range(low, low + tiles):
        here = picked(at_tile(offset, misc_row), index)
        length = jnp.where(owner == (tile + offset + tiles) % tiles, here, length)
    damped = []
    for wave in range(count // 2 + 1):
        basic = 1.0 - math.cos(2.0 * math.pi * wave / count)
        inverse = 1.0 / (1.0 + (2.0 * basic) * length)
        squared = inverse * inverse
        weight = (1.0 if wave in (0, count // 2) else 2.0) / count
        damped.append(squared * squared * weight)
    weights = []
    for gap in range(count // 2 + 1):
        total = None
        for wave in range(count // 2 + 1):
            term = damped[wave] * math.cos(2.0 * math.pi * (wave * gap % count) / count)
            total = term if total is None else total + term
        weights.append(total)

    smooth = [None] * lons
    for offset in range(low, low + tiles):
        for j in range(lons):
            value = at_tile(offset, j)
            for i in range(lons):
                gap = (i - (offset * lons + j)) % count
                term = weights[min(gap, count - gap)] * value
                smooth[i] = term if smooth[i] is None else smooth[i] + term

    lat = lane % lats
    span = lons + 2 * STEPS
    for r in range(span):
        offset, i = (r - STEPS) // lons, (r - STEPS) % lons
        spot = i * group + lane % group
        wind_u = 0.5 * picked(at_tile(offset, 2 * lons), spot)
        wind_v = 0.5 * picked(at_tile(offset, 2 * lons + 1), spot)
        mixing = picked(at_tile(offset, misc_row), i * lats + lat)
        coeff_ref[r, 0] = 1.0 - 4.0 * mixing
        coeff_ref[r, 1] = mixing - wind_u
        coeff_ref[r, 2] = mixing + wind_u
        coeff_ref[r, 3] = jnp.where(lat == lats - 1, 0.0, mixing - wind_v)
        coeff_ref[r, 4] = jnp.where(lat == 0, 0.0, mixing + wind_v)
        edge = at_tile(offset, 2 * lons + 3)
        early = pltpu.roll(edge, (LANES - i * group) % LANES, 1)
        late = pltpu.roll(edge, (2 * LANES - (i + 1) * group) % LANES, 1)
        inside = pltpu.roll(at_tile(offset, lons + i), group, 1)
        field_ref[r] = jnp.where(lane < group, jnp.where(first, 0.0, early), inside)
        inside = pltpu.roll(at_tile(offset, i), LANES - group, 1)
        dual_ref[r] = jnp.where(lane >= LANES - group, jnp.where(first, late, 0.0), inside)

    def north(values):
        return pltpu.roll(values, LANES - 1, 1)

    def south(values):
        return pltpu.roll(values, 1, 1)

    forward = [field_ref[r] for r in range(span)]
    for step in range(STEPS):
        following = []
        for p in range(1, len(forward) - 1):
            r = p + step
            middle = forward[p]
            following.append(
                coeff_ref[r, 0] * middle
                + coeff_ref[r, 1] * forward[p + 1]
                + coeff_ref[r, 2] * forward[p - 1]
                + coeff_ref[r, 3] * north(middle)
                + coeff_ref[r, 4] * south(middle)
            )
        forward = following
    backward = [dual_ref[r] for r in range(span)]
    for step in range(STEPS):
        following = []
        for p in range(1, len(backward) - 1):
            r = p + step
            middle = backward[p]
            following.append(
                coeff_ref[r, 0] * middle
                + coeff_ref[r - 1, 1] * backward[p - 1]
                + coeff_ref[r + 1, 2] * backward[p + 1]
                + south(coeff_ref[r, 3] * middle)
                + north(coeff_ref[r, 4] * middle)
            )
        backward = following

    level = lax.broadcasted_iota(jnp.int32, (SUB, LANES), 0) + SUB * (lane % group // lats)
    scale = jnp.zeros((SUB, LANES), jnp.float32)
    for s in range(wins):
        row = jnp.concatenate(
            [jnp.broadcast_to(spread_ref[s : s + 1, :], (SUB, levels))] * (LANES // levels), axis=1
        )
        scale = jnp.where(lane // group == s, picked(row, level), scale)
    square = scale * scale

    for i in range(lons):
        model = square * smooth[i] + block(0, False, lons + i) - forward[i]
        other = block(0, False, i) - backward[i]
        for s in range(wins):
            for half in range(halves):
                at = (s * halves + half) * lats
                rows = slice(half * SUB, (half + 1) * SUB)
                model_ref[i, s, rows, :] = model[:, at : at + lats]
                dual_out_ref[i, s, rows, :] = other[:, at : at + lats]


def dense_body(increment, dual_vector, wind_u, wind_v, land_sea, length_sq, spread):
    lons, wins, levels, lats = increment.shape
    tiles = lax.axis_size("tiles")
    cores = lax.axis_size("subwin")
    rings = tiles // 2
    main_rows = (2 * lons + 3) * SUB
    vmem = pl.BlockSpec(memory_space=pltpu.VMEM)
    hbm = pl.BlockSpec(memory_space=pltpu.HBM)
    arrays = (increment, dual_vector, wind_u, wind_v, land_sea, length_sq.T)
    main, extra = pl.pallas_call(
        pack_kernel,
        out_shape=(
            jax.ShapeDtypeStruct((main_rows, LANES), jnp.float32),
            jax.ShapeDtypeStruct((SUB, LANES), jnp.float32),
        ),
        in_specs=[hbm] * len(arrays),
        out_specs=(vmem, vmem),
        scratch_shapes=[pltpu.VMEM(x.shape, x.dtype) for x in arrays]
        + [pltpu.SemaphoreType.DMA((len(arrays),))],
        compiler_params=pltpu.CompilerParams(vmem_limit_bytes=VMEM_BYTES),
        name="pack",
    )(*[pltpu.with_memory_space_constraint(x, pltpu.HBM) for x in arrays])

    other = [(w, cores - 1 - w) for w in range(cores)]
    peer = [(t, t ^ 1) for t in range(tiles)]
    across = [
        (t * cores + w, (t ^ 1) * cores + cores - 1 - w) for t in range(tiles) for w in range(cores)
    ]
    swapped = lax.ppermute(extra, "subwin", other)
    peer_main = lax.ppermute(main, "tiles", peer)
    peer_extra = lax.ppermute(extra, ("tiles", "subwin"), across)

    def ring(x, by):
        return lax.ppermute(
            x, "tiles", [(t, (t // 2 + by) % rings * 2 + t % 2) for t in range(tiles)]
        )

    pair = jnp.concatenate([main, swapped, peer_main, peer_extra])
    held, misc = lons * SUB, (2 * lons + 2) * SUB
    short = jnp.concatenate(
        [main[:held], main[misc:], peer_main[:held], peer_main[misc:]]
    )
    left = ring(pair, 1)
    right = ring(pair, -1)
    far = [ring(short, -d) for d in range(2, rings - 1)]
    span = lons + 2 * STEPS
    shape = jax.ShapeDtypeStruct(increment.shape, jnp.float32)
    inputs = [main, swapped, peer_main, peer_extra, left, right, *far, spread]
    return pl.pallas_call(
        functools.partial(apply_kernel, (lons, wins, levels, lats, tiles)),
        out_shape=(shape, shape),
        in_specs=[vmem] * len(inputs),
        out_specs=(vmem, vmem),
        scratch_shapes=[
            pltpu.VMEM((span, 5, SUB, LANES), jnp.float32),
            pltpu.VMEM((span, SUB, LANES), jnp.float32),
            pltpu.VMEM((span, SUB, LANES), jnp.float32),
        ],
        compiler_params=pltpu.CompilerParams(vmem_limit_bytes=VMEM_BYTES),
        name="apply",
    )(*inputs)


def solution(mesh):
    placed = (
        P(("groups", "tiles"), "subwin", None, None),
        P(("groups", "tiles"), "subwin", None, None),
        P("tiles", None, None),
        P("tiles", None, None),
        P("tiles", None),
        P("subwin", "tiles"),
        P("subwin", None),
    )

    def local(*arrays):
        increment = arrays[0]
        lats = increment.shape[3]
        chosen = dense_body if dense_fits(mesh, increment.shape, lats) else body
        return chosen(*arrays)

    return jax.shard_map(
        local,
        mesh=mesh,
        in_specs=placed,
        out_specs=(
            P(("groups", "tiles"), "subwin", None, None),
            P(("groups", "tiles"), "subwin", None, None),
        ),
        check_vma=False,
    )
```

```python
import functools
import math

import jax
import jax.numpy as jnp
from jax import lax
from jax.experimental import pallas as pl
from jax.experimental.pallas import tpu as pltpu
from jax.sharding import PartitionSpec as P


STEPS = 8
SWEEPS = 4
LON_DEV = 4
MODEL_FLOPS = 10**6


def extended(x, sides, width):
    for axis, dim in sides:
        devices, length = (lax.axis_size(axis), x.shape[dim])
        up = [(i, (i + 1) % devices) for i in range(devices)]
        down = [(j, i) for i, j in up]
        last = lax.slice_in_dim(x, length - width, length, axis=dim)
        leading = lax.slice_in_dim(x, 0, width, axis=dim)
        before = lax.ppermute(last, axis, up)
        after = lax.ppermute(leading, axis, down)
        x = jnp.concatenate([before, x, after], axis=dim)
    return x


def passed_along(x, axis, by):
    devices = lax.axis_size(axis)
    pairs = [(i, i + by) for i in range(devices) if 0 <= i + by < devices]
    return lax.ppermute(x, axis, pairs)


def from_north(values):
    return jnp.concatenate([values[..., 1:], jnp.zeros_like(values[..., :1])], axis=-1)


def from_south(values):
    return jnp.concatenate([jnp.zeros_like(values[..., :1]), values[..., :-1]], axis=-1)


def coefficients(wind_u, wind_v, mixing):
    return (
        1.0 - 4.0 * mixing,
        mixing - 0.5 * wind_u,
        mixing + 0.5 * wind_u,
        mixing - 0.5 * wind_v,
        mixing + 0.5 * wind_v,
    )


def tangent_step(fields, coeffs, offset):
    extent = fields.shape[0]
    centre, eastward, westward, northward, southward = [
        coeff[offset + 1 : offset + extent - 1][:, None] for coeff in coeffs
    ]
    middle = fields[1:-1]
    return (
        centre * middle
        + eastward * fields[2:]
        + westward * fields[:-2]
        + northward * from_north(middle)
        + southward * from_south(middle)
    )


def adjoint_step(fields, coeffs, offset):
    extent = fields.shape[0]
    centre = coeffs[0][offset + 1 : offset + extent - 1][:, None]
    northward = coeffs[3][offset + 1 : offset + extent - 1][:, None]
    southward = coeffs[4][offset + 1 : offset + extent - 1][:, None]
    eastward = coeffs[1][offset : offset + extent][:, None]
    westward = coeffs[2][offset : offset + extent][:, None]
    middle = fields[1:-1]
    return (
        centre * middle
        + (eastward * fields)[:-2]
        + (westward * fields)[2:]
        + from_south(northward * middle)
        + from_north(southward * middle)
    )


def run_tangent(fields, coeffs, margin):
    for _ in range(STEPS // margin):
        grown = extended(fields, (("tiles", 0),), margin)
        for _ in range(margin):
            offset = (coeffs[0].shape[0] - grown.shape[0]) // 2
            grown = tangent_step(grown, coeffs, offset)
        fields = grown
    return fields


def run_adjoint(fields, coeffs, margin):
    for _ in range(STEPS // margin):
        grown = extended(fields, (("tiles", 0),), margin)
        for _ in range(margin):
            offset = (coeffs[0].shape[0] - grown.shape[0]) // 2
            grown = adjoint_step(grown, coeffs, offset)
        fields = grown
    return fields


def square_tables(extent):
    index = jnp.arange(extent, dtype=jnp.int32)
    phases = index[:, None] * index[None, :] % extent
    angles = phases.astype(jnp.float32) * (2.0 * math.pi / extent)
    return (jnp.cos(angles), jnp.sin(angles))


def contract(form, first, second):
    return jnp.einsum(form, first, second, precision=lax.Precision.HIGHEST)


def smooth_bands(bands, length_sq):
    count = bands.shape[0]
    inner = LON_DEV
    outer = count // inner
    columns = bands.reshape(outer, inner, -1)
    cos_outer, sin_outer = square_tables(outer)
    cos_inner, sin_inner = square_tables(inner)
    outer_index = jnp.arange(outer, dtype=jnp.int32)
    inner_index = jnp.arange(inner, dtype=jnp.int32)
    twist = (outer_index[:, None] * inner_index[None, :] % count).astype(jnp.float32) * (
        2.0 * math.pi / count
    )
    twist_cos = jnp.cos(twist)[:, :, None]
    twist_sin = jnp.sin(twist)[:, :, None]
    first_real = contract("ab,bqc->aqc", cos_outer, columns)
    first_imag = -contract("ab,bqc->aqc", sin_outer, columns)
    turned_real = first_real * twist_cos + first_imag * twist_sin
    turned_imag = first_imag * twist_cos - first_real * twist_sin
    modes_real = contract("aqc,kq->akc", turned_real, cos_inner) + contract(
        "aqc,kq->akc", turned_imag, sin_inner
    )
    modes_imag = contract("aqc,kq->akc", turned_imag, cos_inner) - contract(
        "aqc,kq->akc", turned_real, sin_inner
    )
    wave = (outer_index[:, None] + outer * inner_index[None, :]).astype(jnp.float32)
    basic = 1.0 - jnp.cos(wave * (2.0 * math.pi / count))
    damping = (1.0 + 2.0 * length_sq[None, None, :, None, :] * basic[:, :, None, None, None]) ** (
        -SWEEPS
    )
    damping = jnp.broadcast_to(damping, (outer, inner) + bands.shape[1:]).reshape(outer, inner, -1)
    modes_real = modes_real * damping
    modes_imag = modes_imag * damping
    back_real = contract("akc,kq->aqc", modes_real, cos_inner) - contract(
        "akc,kq->aqc", modes_imag, sin_inner
    )
    back_imag = contract("akc,kq->aqc", modes_imag, cos_inner) + contract(
        "akc,kq->aqc", modes_real, sin_inner
    )
    final_real = back_real * twist_cos - back_imag * twist_sin
    final_imag = back_imag * twist_cos + back_real * twist_sin
    smoothed = contract("ab,bqc->aqc", cos_outer, final_real) - contract(
        "ab,bqc->aqc", sin_outer, final_imag
    )
    return (smoothed / count).reshape(bands.shape)


def body(increment, dual_vector, wind_u, wind_v, land_sea, length_sq, spread):
    margin = 4
    mixing = 0.15 + 0.09 * land_sea.astype(jnp.float32)
    grown_u, grown_v, grown_mix = (
        extended(wind_u, (("tiles", 0),), margin),
        extended(wind_v, (("tiles", 0),), margin),
        extended(mixing, (("tiles", 0),), margin),
    )
    coeffs = coefficients(grown_u, grown_v, grown_mix[:, None, :])
    carried = passed_along(increment[:, -1:], "subwin", 1)
    previous = jnp.concatenate([carried, increment[:, :-1]], axis=1)
    later = passed_along(dual_vector[:, :1], "subwin", -1)
    following = jnp.concatenate([dual_vector[:, 1:], later], axis=1)
    weighted = dual_vector * spread[None, :, :, None]
    bands = lax.all_to_all(weighted, "tiles", split_axis=3, concat_axis=0, tiled=True)
    smoothed = smooth_bands(bands, length_sq)
    forward = run_tangent(previous, coeffs, margin)
    backward = run_adjoint(following, coeffs, margin)
    returned = lax.all_to_all(smoothed, "tiles", split_axis=0, concat_axis=3, tiled=True)
    covar = returned * spread[None, :, :, None]
    return (covar + increment - forward, dual_vector - backward)


SUB = 8
LANES = 128
VMEM_BYTES = 4 * 2**20


def dense_fits(mesh, shape):
    lons, wins, levels, lats = shape
    tiles = mesh.shape["tiles"]
    halves = levels // SUB
    return (
        levels % SUB == 0
        and wins * halves * lats == LANES
        and lons * halves * lats == LANES
        and LANES % levels == 0
        and lats % tiles == 0
        and lons * lats + wins * (lats // tiles) <= LANES
        and mesh.shape["subwin"] == 2
        and tiles % 2 == 0
        and tiles // 2 >= 4
        and STEPS <= 2 * lons
    )


def lane_index():
    return lax.broadcasted_iota(jnp.int32, (SUB, LANES), 1)


def picked(values, index):
    return jnp.take_along_axis(values, index, axis=1)


class Rows:
    def __init__(self, lons, tiles, main, peer, left, right, far=()):
        self.lons, self.tiles = lons, tiles
        self.even = lax.axis_index("tiles") % 2 == 0
        full = 2 * lons + 3
        whole = {row: row for row in range(full)}
        held = {row: row for row in range(lons)} | {full - 1: lons}
        self.places = ({}, {})
        for odd, sign in enumerate((1, -1)):
            self.add(odd, 0, main, whole, 0)
            self.add(odd, sign, peer, whole, 0)
            for offset, ref in ((-2, left), (2, right)):
                self.add(odd, offset, ref, whole, 0)
                self.add(odd, offset + sign, ref, whole, full)
            for k, ref in enumerate(far):
                self.add(odd, 2 * (k + 2), ref, held, 0)
                self.add(odd, 2 * (k + 2) + sign, ref, held, lons + 1)

    def add(self, odd, offset, ref, rows, start):
        for row, at in rows.items():
            self.places[odd][offset % self.tiles, row] = (ref, (start + at) * SUB)

    def __call__(self, offset, row):
        key = (offset % self.tiles, row)
        (one, at), (two, to) = self.places[0][key], self.places[1][key]
        if one is two and at == to:
            return one[at : at + SUB, :]
        return jnp.where(self.even, one[at : at + SUB, :], two[to : to + SUB, :])


def pack_kernel(*refs):
    arrays, main_ref, held, arrived = refs[:6], refs[6], refs[7:13], refs[13]
    copies = [
        pltpu.make_async_copy(source, target, arrived.at[k])
        for k, (source, target) in enumerate(zip(arrays, held))
    ]
    for copy in copies:
        copy.start()
    for copy in copies:
        copy.wait()
    inc_ref, dual_ref, u_ref, v_ref, land_ref, len_ref = held
    lons, wins, levels, lats = inc_ref.shape
    halves = levels // SUB
    own_lats = len_ref.shape[0]

    def put(row, slot, value):
        main_ref[row * SUB : (row + 1) * SUB, slot * lats : (slot + 1) * lats] = value

    for i in range(lons):
        for half in range(halves):
            rows = slice(half * SUB, (half + 1) * SUB)
            for s in range(wins):
                put(i, s * halves + half, dual_ref[i, s, rows, :])
                put(lons + i, s * halves + half, inc_ref[i, s, rows, :])
            put(2 * lons, i * halves + half, u_ref[i, rows, :])
            put(2 * lons + 1, i * halves + half, v_ref[i, rows, :])
    base = (2 * lons + 2) * SUB
    main_ref[base : base + SUB, :] = jnp.zeros((SUB, LANES), jnp.float32)
    for i in range(lons):
        mixing = 0.15 + 0.09 * land_ref[i : i + 1, :].astype(jnp.float32)
        main_ref[base : base + SUB, i * lats : (i + 1) * lats] = jnp.broadcast_to(mixing, (SUB, lats))
    for j in range(own_lats):
        at = lons * lats + j * wins
        main_ref[base : base + SUB, at : at + wins] = jnp.broadcast_to(
            len_ref[j : j + 1, :], (SUB, wins)
        )


def model_kernel(geometry, main, peer, left, right, forward_ref, backward_ref, edge_ref, coeff_ref):
    lons, wins, _, lats, tiles = geometry
    group = LANES // wins
    rows = Rows(lons, tiles, main, peer, left, right)
    lane = lane_index()
    lat = lane % lats
    span = lons + 2 * STEPS
    forward, backward = [], []
    for r in range(span):
        offset, i = (r - STEPS) // lons, (r - STEPS) % lons
        spot = i * group + lane % group
        wind_u = 0.5 * picked(rows(offset, 2 * lons), spot)
        wind_v = 0.5 * picked(rows(offset, 2 * lons + 1), spot)
        mixing = picked(rows(offset, 2 * lons + 2), i * lats + lat)
        coeff_ref[r, 0] = 1.0 - 4.0 * mixing
        coeff_ref[r, 1] = mixing - wind_u
        coeff_ref[r, 2] = mixing + wind_u
        coeff_ref[r, 3] = jnp.where(lat == lats - 1, 0.0, mixing - wind_v)
        coeff_ref[r, 4] = jnp.where(lat == 0, 0.0, mixing + wind_v)
        forward.append(rows(offset, lons + i))
        backward.append(rows(offset, i))

    def north(values):
        return pltpu.roll(values, LANES - 1, 1)

    def south(values):
        return pltpu.roll(values, 1, 1)

    for step in range(STEPS):
        ahead, behind = [], []
        for p in range(1, len(forward) - 1):
            r = p + step
            middle = forward[p]
            ahead.append(
                coeff_ref[r, 0] * middle
                + coeff_ref[r, 1] * forward[p + 1]
                + coeff_ref[r, 2] * forward[p - 1]
                + coeff_ref[r, 3] * north(middle)
                + coeff_ref[r, 4] * south(middle)
            )
            middle = backward[p]
            behind.append(
                coeff_ref[r, 0] * middle
                + coeff_ref[r - 1, 1] * backward[p - 1]
                + coeff_ref[r + 1, 2] * backward[p + 1]
                + south(coeff_ref[r, 3] * middle)
                + north(coeff_ref[r, 4] * middle)
            )
        forward, backward = ahead, behind
    first = lax.axis_index("subwin") == 0
    for i in range(lons):
        at = slice(i * SUB, (i + 1) * SUB)
        forward_ref[at, :] = forward[i]
        backward_ref[at, :] = backward[i]
        edge_ref[at, :] = jnp.where(first, forward[i], backward[i])


def unpack(ref, i, value, wins, halves, lats):
    for s in range(wins):
        for half in range(halves):
            at = (s * halves + half) * lats
            ref[i, s, half * SUB : (half + 1) * SUB, :] = value[:, at : at + lats]


def finish_kernel(geometry, *refs):
    lons, wins, levels, lats, tiles = geometry
    group = LANES // wins
    own_lats = lats // tiles
    count = lons * tiles
    main, peer, left, right = refs[:4]
    far, (forward_ref, backward_ref, edge_ref, spread_ref) = refs[4:-9], refs[-9:-5]
    model_ref, dual_out_ref, model_held, dual_held, sent = refs[-5:]
    first = lax.axis_index("subwin") == 0
    rows = Rows(lons, tiles, main, peer, left, right, far)
    lane = lane_index()
    tile = lax.axis_index("tiles")

    rest = []
    for i in range(lons):
        at = slice(i * SUB, (i + 1) * SUB)
        edge = edge_ref[at, :]
        ahead = jnp.where(lane < LANES - group, forward_ref[at, :], jnp.where(first, 0.0, edge))
        behind = jnp.where(lane >= group, backward_ref[at, :], jnp.where(first, edge, 0.0))
        rest.append(rows(0, lons + i) - pltpu.roll(ahead, group, 1))
        dual_side = rows(0, i) - pltpu.roll(behind, LANES - group, 1)
        unpack(dual_held, i, dual_side, wins, levels // SUB, lats)
    dual_copy = pltpu.make_async_copy(dual_held, dual_out_ref, sent.at[0])
    dual_copy.start()

    length = jnp.zeros((SUB, LANES), jnp.float32)
    index = lons * lats + wins * (lane % own_lats) + lane // group
    owner = lane % lats // own_lats
    for offset in range(tiles):
        here = picked(rows(offset, 2 * lons + 2), index)
        length = jnp.where(owner == (tile + offset) % tiles, here, length)
    half = count // 2
    damped = []
    for wave in range(half + 1):
        basic = 1.0 - math.cos(2.0 * math.pi * wave / count)
        inverse = 1.0 / (1.0 + (2.0 * basic) * length)
        squared = inverse * inverse
        weight = (1.0 if wave in (0, half) else 2.0) / count
        damped.append(squared * (squared * weight))

    def waves(gap, start):
        total = None
        for wave in range(start, half + 1, 2):
            factor = math.cos(2.0 * math.pi * (wave * gap % count) / count)
            term = damped[wave] if factor == 1.0 else damped[wave] * factor
            total = term if total is None else total + term
        return total

    weights = [None] * (half + 1)
    for gap in range(half // 2 + 1):
        even, odd = waves(gap, 0), waves(gap, 1)
        weights[gap] = even + odd
        weights[half - gap] = even - odd if half % 2 == 0 else None
    for gap in range(half + 1):
        if weights[gap] is None:
            weights[gap] = waves(gap, 0) + waves(gap, 1)

    smooth = [None] * lons
    for offset in range(tiles):
        for j in range(lons):
            value = rows(offset, j)
            for i in range(lons):
                gap = (i - (offset * lons + j)) % count
                term = weights[min(gap, count - gap)] * value
                smooth[i] = term if smooth[i] is None else smooth[i] + term

    level = lax.broadcasted_iota(jnp.int32, (SUB, LANES), 0) + SUB * (lane % group // lats)
    scale = jnp.zeros((SUB, LANES), jnp.float32)
    for s in range(wins):
        row = jnp.concatenate(
            [jnp.broadcast_to(spread_ref[s : s + 1, :], (SUB, levels))] * (LANES // levels), axis=1
        )
        scale = jnp.where(lane // group == s, picked(row, level), scale)
    square = scale * scale
    for i in range(lons):
        unpack(model_held, i, square * smooth[i] + rest[i], wins, levels // SUB, lats)
    model_copy = pltpu.make_async_copy(model_held, model_ref, sent.at[1])
    model_copy.start()
    dual_copy.wait()
    model_copy.wait()


def kernel_call(kernel, inputs, outputs, scratch=(), flops=0, space=pltpu.VMEM):
    vmem = pl.BlockSpec(memory_space=pltpu.VMEM)
    return pl.pallas_call(
        kernel,
        out_shape=outputs,
        in_specs=[vmem] * len(inputs),
        out_specs=(pl.BlockSpec(memory_space=space),) * len(outputs),
        scratch_shapes=list(scratch),
        compiler_params=pltpu.CompilerParams(vmem_limit_bytes=VMEM_BYTES),
        cost_estimate=pl.CostEstimate(flops=flops, bytes_accessed=2**18, transcendentals=0),
    )(*inputs)


def dense_body(increment, dual_vector, wind_u, wind_v, land_sea, length_sq, spread):
    lons, wins, levels, lats = increment.shape
    tiles = lax.axis_size("tiles")
    rings = tiles // 2
    geometry = (lons, wins, levels, lats, tiles)

    def rows(count):
        return jax.ShapeDtypeStruct((count * SUB, LANES), jnp.float32)

    full = jax.ShapeDtypeStruct(increment.shape, jnp.float32)
    arrays = (increment, dual_vector, wind_u, wind_v, land_sea, length_sq.T)
    main = pl.pallas_call(
        pack_kernel,
        out_shape=rows(2 * lons + 3),
        in_specs=[pl.BlockSpec(memory_space=pltpu.HBM)] * len(arrays),
        out_specs=pl.BlockSpec(memory_space=pltpu.VMEM),
        scratch_shapes=[pltpu.VMEM(x.shape, x.dtype) for x in arrays]
        + [pltpu.SemaphoreType.DMA((len(arrays),))],
        compiler_params=pltpu.CompilerParams(vmem_limit_bytes=VMEM_BYTES),
        name="pack",
    )(*[pltpu.with_memory_space_constraint(x, pltpu.HBM) for x in arrays])

    def moved(x, by):
        pairs = [(t, (t // 2 + by) % rings * 2 + t % 2) for t in range(tiles)]
        return lax.ppermute(x, "tiles", pairs)

    peer = lax.ppermute(main, "tiles", [(t, t ^ 1) for t in range(tiles)])
    held, misc = lons * SUB, (2 * lons + 2) * SUB
    pair = jnp.concatenate([main, peer])
    left = moved(pair, 1)
    right = moved(pair, -1)
    short = jnp.concatenate([main[:held], main[misc:], peer[:held], peer[misc:]])
    far = [moved(short, -d) for d in range(2, rings - 1)]
    near = (main, peer, left, right)
    forward, backward, edge = kernel_call(
        functools.partial(model_kernel, geometry),
        near,
        (rows(lons), rows(lons), rows(lons)),
        [pltpu.VMEM((lons + 2 * STEPS, 5, SUB, LANES), jnp.float32)],
        flops=MODEL_FLOPS,
    )
    edge = lax.ppermute(edge, "subwin", [(0, 1), (1, 0)])
    model_side, dual_side = kernel_call(
        functools.partial(finish_kernel, geometry),
        (*near, *far, forward, backward, edge, spread),
        (full, full),
        [pltpu.VMEM(full.shape, full.dtype)] * 2 + [pltpu.SemaphoreType.DMA((2,))],
        flops=MODEL_FLOPS,
        space=pltpu.HBM,
    )
    return model_side, dual_side


def solution(mesh):
    placed = (
        P(("groups", "tiles"), "subwin", None, None),
        P(("groups", "tiles"), "subwin", None, None),
        P("tiles", None, None),
        P("tiles", None, None),
        P("tiles", None),
        P("subwin", "tiles"),
        P("subwin", None),
    )

    def local(*arrays):
        if dense_fits(mesh, arrays[0].shape):
            return dense_body(*arrays)
        return body(*arrays)

    return jax.shard_map(
        local,
        mesh=mesh,
        in_specs=placed,
        out_specs=(
            P(("groups", "tiles"), "subwin", None, None),
            P(("groups", "tiles"), "subwin", None, None),
        ),
        check_vma=False,
    )
```

```python
import functools
import math

import jax
import jax.numpy as jnp
from jax import lax
from jax.experimental import pallas as pl
from jax.experimental.pallas import tpu as pltpu
from jax.sharding import PartitionSpec as P


STEPS = 8
SWEEPS = 4
LON_DEV = 4
MODEL_FLOPS = 10**6


def extended(x, sides, width):
    for axis, dim in sides:
        devices, length = (lax.axis_size(axis), x.shape[dim])
        up = [(i, (i + 1) % devices) for i in range(devices)]
        down = [(j, i) for i, j in up]
        last = lax.slice_in_dim(x, length - width, length, axis=dim)
        leading = lax.slice_in_dim(x, 0, width, axis=dim)
        before = lax.ppermute(last, axis, up)
        after = lax.ppermute(leading, axis, down)
        x = jnp.concatenate([before, x, after], axis=dim)
    return x


def passed_along(x, axis, by):
    devices = lax.axis_size(axis)
    pairs = [(i, i + by) for i in range(devices) if 0 <= i + by < devices]
    return lax.ppermute(x, axis, pairs)


def from_north(values):
    return jnp.concatenate([values[..., 1:], jnp.zeros_like(values[..., :1])], axis=-1)


def from_south(values):
    return jnp.concatenate([jnp.zeros_like(values[..., :1]), values[..., :-1]], axis=-1)


def coefficients(wind_u, wind_v, mixing):
    return (
        1.0 - 4.0 * mixing,
        mixing - 0.5 * wind_u,
        mixing + 0.5 * wind_u,
        mixing - 0.5 * wind_v,
        mixing + 0.5 * wind_v,
    )


def tangent_step(fields, coeffs, offset):
    extent = fields.shape[0]
    centre, eastward, westward, northward, southward = [
        coeff[offset + 1 : offset + extent - 1][:, None] for coeff in coeffs
    ]
    middle = fields[1:-1]
    return (
        centre * middle
        + eastward * fields[2:]
        + westward * fields[:-2]
        + northward * from_north(middle)
        + southward * from_south(middle)
    )


def adjoint_step(fields, coeffs, offset):
    extent = fields.shape[0]
    centre = coeffs[0][offset + 1 : offset + extent - 1][:, None]
    northward = coeffs[3][offset + 1 : offset + extent - 1][:, None]
    southward = coeffs[4][offset + 1 : offset + extent - 1][:, None]
    eastward = coeffs[1][offset : offset + extent][:, None]
    westward = coeffs[2][offset : offset + extent][:, None]
    middle = fields[1:-1]
    return (
        centre * middle
        + (eastward * fields)[:-2]
        + (westward * fields)[2:]
        + from_south(northward * middle)
        + from_north(southward * middle)
    )


def run_tangent(fields, coeffs, margin):
    for _ in range(STEPS // margin):
        grown = extended(fields, (("tiles", 0),), margin)
        for _ in range(margin):
            offset = (coeffs[0].shape[0] - grown.shape[0]) // 2
            grown = tangent_step(grown, coeffs, offset)
        fields = grown
    return fields


def run_adjoint(fields, coeffs, margin):
    for _ in range(STEPS // margin):
        grown = extended(fields, (("tiles", 0),), margin)
        for _ in range(margin):
            offset = (coeffs[0].shape[0] - grown.shape[0]) // 2
            grown = adjoint_step(grown, coeffs, offset)
        fields = grown
    return fields


def square_tables(extent):
    index = jnp.arange(extent, dtype=jnp.int32)
    phases = index[:, None] * index[None, :] % extent
    angles = phases.astype(jnp.float32) * (2.0 * math.pi / extent)
    return (jnp.cos(angles), jnp.sin(angles))


def contract(form, first, second):
    return jnp.einsum(form, first, second, precision=lax.Precision.HIGHEST)


def smooth_bands(bands, length_sq):
    count = bands.shape[0]
    inner = LON_DEV
    outer = count // inner
    columns = bands.reshape(outer, inner, -1)
    cos_outer, sin_outer = square_tables(outer)
    cos_inner, sin_inner = square_tables(inner)
    outer_index = jnp.arange(outer, dtype=jnp.int32)
    inner_index = jnp.arange(inner, dtype=jnp.int32)
    twist = (outer_index[:, None] * inner_index[None, :] % count).astype(jnp.float32) * (
        2.0 * math.pi / count
    )
    twist_cos = jnp.cos(twist)[:, :, None]
    twist_sin = jnp.sin(twist)[:, :, None]
    first_real = contract("ab,bqc->aqc", cos_outer, columns)
    first_imag = -contract("ab,bqc->aqc", sin_outer, columns)
    turned_real = first_real * twist_cos + first_imag * twist_sin
    turned_imag = first_imag * twist_cos - first_real * twist_sin
    modes_real = contract("aqc,kq->akc", turned_real, cos_inner) + contract(
        "aqc,kq->akc", turned_imag, sin_inner
    )
    modes_imag = contract("aqc,kq->akc", turned_imag, cos_inner) - contract(
        "aqc,kq->akc", turned_real, sin_inner
    )
    wave = (outer_index[:, None] + outer * inner_index[None, :]).astype(jnp.float32)
    basic = 1.0 - jnp.cos(wave * (2.0 * math.pi / count))
    damping = (1.0 + 2.0 * length_sq[None, None, :, None, :] * basic[:, :, None, None, None]) ** (
        -SWEEPS
    )
    damping = jnp.broadcast_to(damping, (outer, inner) + bands.shape[1:]).reshape(outer, inner, -1)
    modes_real = modes_real * damping
    modes_imag = modes_imag * damping
    back_real = contract("akc,kq->aqc", modes_real, cos_inner) - contract(
        "akc,kq->aqc", modes_imag, sin_inner
    )
    back_imag = contract("akc,kq->aqc", modes_imag, cos_inner) + contract(
        "akc,kq->aqc", modes_real, sin_inner
    )
    final_real = back_real * twist_cos - back_imag * twist_sin
    final_imag = back_imag * twist_cos + back_real * twist_sin
    smoothed = contract("ab,bqc->aqc", cos_outer, final_real) - contract(
        "ab,bqc->aqc", sin_outer, final_imag
    )
    return (smoothed / count).reshape(bands.shape)


def body(increment, dual_vector, wind_u, wind_v, land_sea, length_sq, spread):
    margin = 4
    mixing = 0.15 + 0.09 * land_sea.astype(jnp.float32)
    grown_u, grown_v, grown_mix = (
        extended(wind_u, (("tiles", 0),), margin),
        extended(wind_v, (("tiles", 0),), margin),
        extended(mixing, (("tiles", 0),), margin),
    )
    coeffs = coefficients(grown_u, grown_v, grown_mix[:, None, :])
    carried = passed_along(increment[:, -1:], "subwin", 1)
    previous = jnp.concatenate([carried, increment[:, :-1]], axis=1)
    later = passed_along(dual_vector[:, :1], "subwin", -1)
    following = jnp.concatenate([dual_vector[:, 1:], later], axis=1)
    weighted = dual_vector * spread[None, :, :, None]
    bands = lax.all_to_all(weighted, "tiles", split_axis=3, concat_axis=0, tiled=True)
    smoothed = smooth_bands(bands, length_sq)
    forward = run_tangent(previous, coeffs, margin)
    backward = run_adjoint(following, coeffs, margin)
    returned = lax.all_to_all(smoothed, "tiles", split_axis=0, concat_axis=3, tiled=True)
    covar = returned * spread[None, :, :, None]
    return (covar + increment - forward, dual_vector - backward)


SUB = 8
LANES = 128
VMEM_BYTES = 4 * 2**20


def dense_fits(mesh, shape):
    lons, wins, levels, lats = shape
    tiles = mesh.shape["tiles"]
    halves = levels // SUB
    return (
        levels % SUB == 0
        and wins * halves * lats == LANES
        and lons * halves * lats == LANES
        and LANES % levels == 0
        and lats % tiles == 0
        and lons * lats + wins * (lats // tiles) <= LANES
        and mesh.shape["subwin"] == 2
        and tiles % 2 == 0
        and tiles // 2 >= 4
        and STEPS <= 2 * lons
    )


def lane_index():
    return lax.broadcasted_iota(jnp.int32, (SUB, LANES), 1)


def picked(values, index):
    return jnp.take_along_axis(values, index, axis=1)


class Rows:
    def __init__(self, lons, tiles, main, peer, left=None, right=None, far=()):
        self.tiles = tiles
        self.even = lax.axis_index("tiles") % 2 == 0
        full = 2 * lons + 3
        whole = {row - 1: row * SUB for row in range(full)}
        held = {row - 1: row * SUB for row in range(lons + 1)}
        self.places = ({}, {})
        for odd, sign in enumerate((1, -1)):
            self.add(odd, 0, main, whole, 0, 0)
            self.add(odd, sign, peer, whole, 0, 0)
            for offset, ref in ((-2, left), (2, right)):
                self.add(odd, offset, ref, whole, 0, 0)
                self.add(odd, offset + sign, ref, whole, full - 1, SUB // 2)
            for k, ref in enumerate(far):
                self.add(odd, 2 * (k + 2), ref, held, 0, 0)
                self.add(odd, 2 * (k + 2) + sign, ref, held, lons, SUB // 2)

    def add(self, odd, offset, ref, rows, start, misc):
        for row, at in rows.items():
            at = misc if row < 0 else start * SUB + at
            self.places[odd][offset % self.tiles, row] = (ref, at)

    def __call__(self, offset, row):
        key = (offset % self.tiles, row)
        places = [self.places[odd][key] for odd in (0, 1)]
        if row < 0:
            values = [jnp.broadcast_to(ref[at : at + 1, :], (SUB, LANES)) for ref, at in places]
        else:
            values = [ref[at : at + SUB, :] for ref, at in places]
        if places[0][0] is places[1][0] and places[0][1] == places[1][1]:
            return values[0]
        return jnp.where(self.even, values[0], values[1])


def pack_kernel(*refs):
    arrays, main_ref, held, arrived = refs[:6], refs[6], refs[7:13], refs[13]
    copies = [
        pltpu.make_async_copy(source, target, arrived.at[k])
        for k, (source, target) in enumerate(zip(arrays, held))
    ]
    for copy in copies:
        copy.start()
    for copy in copies:
        copy.wait()
    inc_ref, dual_ref, u_ref, v_ref, land_ref, len_ref = held
    lons, wins, levels, lats = inc_ref.shape
    halves = levels // SUB
    own_lats = len_ref.shape[0]

    def put(row, slot, value):
        at = (row + 1) * SUB
        main_ref[at : at + SUB, slot * lats : (slot + 1) * lats] = value

    for i in range(lons):
        for half in range(halves):
            rows = slice(half * SUB, (half + 1) * SUB)
            for s in range(wins):
                put(i, s * halves + half, dual_ref[i, s, rows, :])
                put(lons + i, s * halves + half, inc_ref[i, s, rows, :])
            put(2 * lons, i * halves + half, u_ref[i, rows, :])
            put(2 * lons + 1, i * halves + half, v_ref[i, rows, :])
    main_ref[:SUB, :] = jnp.zeros((SUB, LANES), jnp.float32)
    for i in range(lons):
        mixing = 0.15 + 0.09 * land_ref[i : i + 1, :].astype(jnp.float32)
        main_ref[:SUB, i * lats : (i + 1) * lats] = jnp.broadcast_to(mixing, (SUB, lats))
    for j in range(own_lats):
        at = lons * lats + j * wins
        main_ref[:SUB, at : at + wins] = jnp.broadcast_to(
            len_ref[j : j + 1, :], (SUB, wins)
        )


def north(values):
    return pltpu.roll(values, LANES - 1, 1)


def south(values):
    return pltpu.roll(values, 1, 1)


def model_kernel(geometry, *refs):
    lons, wins, _, lats, tiles = geometry
    near, (forward_ref, backward_ref, edge_ref, coeff_ref) = refs[:-4], refs[-4:]
    group = LANES // wins
    rows = Rows(lons, tiles, *near)
    lane = lane_index()
    lat = lane % lats
    forward, backward = [], []
    for r in range(lons + 2 * STEPS):
        offset, i = (r - STEPS) // lons, (r - STEPS) % lons
        spot = i * group + lane % group
        wind_u = 0.5 * picked(rows(offset, 2 * lons), spot)
        wind_v = 0.5 * picked(rows(offset, 2 * lons + 1), spot)
        mixing = picked(rows(offset, -1), i * lats + lat)
        coeff_ref[r, 0] = 1.0 - 4.0 * mixing
        coeff_ref[r, 1] = mixing - wind_u
        coeff_ref[r, 2] = mixing + wind_u
        coeff_ref[r, 3] = jnp.where(lat == lats - 1, 0.0, mixing - wind_v)
        coeff_ref[r, 4] = jnp.where(lat == 0, 0.0, mixing + wind_v)
        forward.append(rows(offset, lons + i))
        backward.append(rows(offset, i))
    for step in range(STEPS):
        ahead, behind = [], []
        for p in range(1, len(forward) - 1):
            r = p + step
            middle = forward[p]
            ahead.append(
                coeff_ref[r, 0] * middle
                + coeff_ref[r, 1] * forward[p + 1]
                + coeff_ref[r, 2] * forward[p - 1]
                + coeff_ref[r, 3] * north(middle)
                + coeff_ref[r, 4] * south(middle)
            )
            middle = backward[p]
            behind.append(
                coeff_ref[r, 0] * middle
                + coeff_ref[r - 1, 1] * backward[p - 1]
                + coeff_ref[r + 1, 2] * backward[p + 1]
                + south(coeff_ref[r, 3] * middle)
                + north(coeff_ref[r, 4] * middle)
            )
        forward, backward = ahead, behind
    first = lax.axis_index("subwin") == 0
    for i in range(lons):
        at = slice(i * SUB, (i + 1) * SUB)
        forward_ref[at, :] = forward[i]
        backward_ref[at, :] = backward[i]
        edge_ref[at, :] = jnp.where(first, forward[i], backward[i])


def unpack(ref, i, value, wins, halves, lats):
    for s in range(wins):
        for half in range(halves):
            at = (s * halves + half) * lats
            ref[i, s, half * SUB : (half + 1) * SUB, :] = value[:, at : at + lats]


def filter_kernel(geometry, *refs):
    lons, wins, levels, lats, tiles = geometry
    group = LANES // wins
    own_lats = lats // tiles
    count = lons * tiles
    main, peer, left, right = refs[:4]
    far, (spread_ref, covar_ref) = refs[4:-2], refs[-2:]
    rows = Rows(lons, tiles, main, peer, left, right, far)
    lane = lane_index()
    tile = lax.axis_index("tiles")

    length = jnp.zeros((SUB, LANES), jnp.float32)
    index = lons * lats + wins * (lane % own_lats) + lane // group
    owner = lane % lats // own_lats
    for offset in range(tiles):
        here = picked(rows(offset, -1), index)
        length = jnp.where(owner == (tile + offset) % tiles, here, length)
    half = count // 2
    damped = []
    for wave in range(half + 1):
        basic = 1.0 - math.cos(2.0 * math.pi * wave / count)
        inverse = 1.0 / (1.0 + (2.0 * basic) * length)
        squared = inverse * inverse
        weight = (1.0 if wave in (0, half) else 2.0) / count
        damped.append(squared * (squared * weight))

    def waves(gap, start):
        total = None
        for wave in range(start, half + 1, 2):
            factor = math.cos(2.0 * math.pi * (wave * gap % count) / count)
            term = damped[wave] if factor == 1.0 else damped[wave] * factor
            total = term if total is None else total + term
        return total

    weights = [None] * (half + 1)
    for gap in range(half // 2 + 1):
        even, odd = waves(gap, 0), waves(gap, 1)
        weights[gap] = even + odd
        weights[half - gap] = even - odd if half % 2 == 0 else None
    for gap in range(half + 1):
        if weights[gap] is None:
            weights[gap] = waves(gap, 0) + waves(gap, 1)

    smooth = [None] * lons
    for offset in range(tiles):
        for j in range(lons):
            value = rows(offset, j)
            for i in range(lons):
                gap = (i - (offset * lons + j)) % count
                term = weights[min(gap, count - gap)] * value
                smooth[i] = term if smooth[i] is None else smooth[i] + term

    level = lax.broadcasted_iota(jnp.int32, (SUB, LANES), 0) + SUB * (lane % group // lats)
    scale = jnp.zeros((SUB, LANES), jnp.float32)
    for s in range(wins):
        row = jnp.concatenate(
            [jnp.broadcast_to(spread_ref[s : s + 1, :], (SUB, levels))] * (LANES // levels), axis=1
        )
        scale = jnp.where(lane // group == s, picked(row, level), scale)
    square = scale * scale
    for i in range(lons):
        covar_ref[i * SUB : (i + 1) * SUB, :] = square * smooth[i]


def finish_kernel(geometry, *refs):
    lons, wins, levels, lats, _ = geometry
    main, forward_ref, backward_ref, swapped_ref, covar_ref = refs[:5]
    outs, held, sent = refs[5:7], refs[7:9], refs[9]
    group = LANES // wins
    lane = lane_index()
    first = lax.axis_index("subwin") == 0
    copies = [pltpu.make_async_copy(held[k], outs[k], sent.at[k]) for k in (0, 1)]
    for i in range(lons):
        at = slice(i * SUB, (i + 1) * SUB)
        edge = jnp.where(first, swapped_ref[at, :], 0.0)
        behind = jnp.where(lane >= group, backward_ref[at, :], edge)
        value = main[(i + 1) * SUB : (i + 2) * SUB, :] - pltpu.roll(behind, LANES - group, 1)
        unpack(held[1], i, value, wins, levels // SUB, lats)
    copies[1].start()
    for i in range(lons):
        at = slice(i * SUB, (i + 1) * SUB)
        edge = jnp.where(first, 0.0, swapped_ref[at, :])
        ahead = jnp.where(lane < LANES - group, forward_ref[at, :], edge)
        increment = main[(lons + i + 1) * SUB : (lons + i + 2) * SUB, :]
        value = covar_ref[at, :] + increment - pltpu.roll(ahead, group, 1)
        unpack(held[0], i, value, wins, levels // SUB, lats)
    copies[0].start()
    for copy in copies:
        copy.wait()


def kernel_call(kernel, inputs, outputs, scratch=(), flops=0, space=pltpu.VMEM):
    vmem = pl.BlockSpec(memory_space=pltpu.VMEM)
    return pl.pallas_call(
        kernel,
        out_shape=outputs,
        in_specs=[vmem] * len(inputs),
        out_specs=(pl.BlockSpec(memory_space=space),) * len(outputs),
        scratch_shapes=list(scratch),
        compiler_params=pltpu.CompilerParams(vmem_limit_bytes=VMEM_BYTES),
        cost_estimate=pl.CostEstimate(flops=flops, bytes_accessed=2**18, transcendentals=0),
    )(*inputs)


def dense_body(increment, dual_vector, wind_u, wind_v, land_sea, length_sq, spread):
    lons, wins, levels, lats = increment.shape
    tiles = lax.axis_size("tiles")
    rings = tiles // 2
    geometry = (lons, wins, levels, lats, tiles)

    def rows(count):
        return jax.ShapeDtypeStruct((count * SUB, LANES), jnp.float32)

    full = jax.ShapeDtypeStruct(increment.shape, jnp.float32)
    arrays = (increment, dual_vector, wind_u, wind_v, land_sea, length_sq.T)
    main = pl.pallas_call(
        pack_kernel,
        out_shape=rows(2 * lons + 3),
        in_specs=[pl.BlockSpec(memory_space=pltpu.HBM)] * len(arrays),
        out_specs=pl.BlockSpec(memory_space=pltpu.VMEM),
        scratch_shapes=[pltpu.VMEM(x.shape, x.dtype) for x in arrays]
        + [pltpu.SemaphoreType.DMA((len(arrays),))],
        compiler_params=pltpu.CompilerParams(vmem_limit_bytes=VMEM_BYTES),
        name="pack",
    )(*[pltpu.with_memory_space_constraint(x, pltpu.HBM) for x in arrays])

    def moved(x, by):
        pairs = [(t, (t // 2 + by) % rings * 2 + t % 2) for t in range(tiles)]
        return lax.ppermute(x, "tiles", pairs)

    peer = lax.ppermute(main, "tiles", [(t, t ^ 1) for t in range(tiles)])
    row = lax.broadcasted_iota(jnp.int32, (SUB, LANES), 0)
    misc = jnp.where(row < SUB // 2, main[:SUB], peer[:SUB])
    held = (lons + 1) * SUB
    pair = jnp.concatenate([misc, main[SUB:], peer[SUB:]])
    left = moved(pair, 1)
    right = moved(pair, -1)
    short = jnp.concatenate([misc, main[SUB:held], peer[SUB:held]])
    far = [moved(short, -d) for d in range(2, rings - 1)]
    near = (main, peer, left, right)
    span = lons + 2 * STEPS
    forward, backward, edge = kernel_call(
        functools.partial(model_kernel, geometry),
        near,
        (rows(lons),) * 3,
        [pltpu.VMEM((span, 5, SUB, LANES), jnp.float32)],
        flops=MODEL_FLOPS,
    )
    swapped = lax.ppermute(edge, "subwin", [(0, 1), (1, 0)])
    (covar,) = kernel_call(
        functools.partial(filter_kernel, geometry),
        (*near, *far, spread),
        (rows(lons),),
        flops=MODEL_FLOPS,
    )
    model_side, dual_side = kernel_call(
        functools.partial(finish_kernel, geometry),
        (main, forward, backward, swapped, covar),
        (full, full),
        [pltpu.VMEM(full.shape, full.dtype)] * 2 + [pltpu.SemaphoreType.DMA((2,))],
        flops=MODEL_FLOPS,
        space=pltpu.HBM,
    )
    return model_side, dual_side


def solution(mesh):
    placed = (
        P(("groups", "tiles"), "subwin", None, None),
        P(("groups", "tiles"), "subwin", None, None),
        P("tiles", None, None),
        P("tiles", None, None),
        P("tiles", None),
        P("subwin", "tiles"),
        P("subwin", None),
    )

    def local(*arrays):
        if dense_fits(mesh, arrays[0].shape):
            return dense_body(*arrays)
        return body(*arrays)

    return jax.shard_map(
        local,
        mesh=mesh,
        in_specs=placed,
        out_specs=(
            P(("groups", "tiles"), "subwin", None, None),
            P(("groups", "tiles"), "subwin", None, None),
        ),
        check_vma=False,
    )
```

```python
import functools
import math

import jax
import jax.numpy as jnp
from jax import lax
from jax.experimental import pallas as pl
from jax.experimental.pallas import tpu as pltpu
from jax.sharding import PartitionSpec as P


STEPS = 8
SWEEPS = 4
LON_DEV = 4
MODEL_FLOPS = 10**6


def extended(x, sides, width):
    for axis, dim in sides:
        devices, length = (lax.axis_size(axis), x.shape[dim])
        up = [(i, (i + 1) % devices) for i in range(devices)]
        down = [(j, i) for i, j in up]
        last = lax.slice_in_dim(x, length - width, length, axis=dim)
        leading = lax.slice_in_dim(x, 0, width, axis=dim)
        before = lax.ppermute(last, axis, up)
        after = lax.ppermute(leading, axis, down)
        x = jnp.concatenate([before, x, after], axis=dim)
    return x


def passed_along(x, axis, by):
    devices = lax.axis_size(axis)
    pairs = [(i, i + by) for i in range(devices) if 0 <= i + by < devices]
    return lax.ppermute(x, axis, pairs)


def from_north(values):
    return jnp.concatenate([values[..., 1:], jnp.zeros_like(values[..., :1])], axis=-1)


def from_south(values):
    return jnp.concatenate([jnp.zeros_like(values[..., :1]), values[..., :-1]], axis=-1)


def coefficients(wind_u, wind_v, mixing):
    return (
        1.0 - 4.0 * mixing,
        mixing - 0.5 * wind_u,
        mixing + 0.5 * wind_u,
        mixing - 0.5 * wind_v,
        mixing + 0.5 * wind_v,
    )


def tangent_step(fields, coeffs, offset):
    extent = fields.shape[0]
    centre, eastward, westward, northward, southward = [
        coeff[offset + 1 : offset + extent - 1][:, None] for coeff in coeffs
    ]
    middle = fields[1:-1]
    return (
        centre * middle
        + eastward * fields[2:]
        + westward * fields[:-2]
        + northward * from_north(middle)
        + southward * from_south(middle)
    )


def adjoint_step(fields, coeffs, offset):
    extent = fields.shape[0]
    centre = coeffs[0][offset + 1 : offset + extent - 1][:, None]
    northward = coeffs[3][offset + 1 : offset + extent - 1][:, None]
    southward = coeffs[4][offset + 1 : offset + extent - 1][:, None]
    eastward = coeffs[1][offset : offset + extent][:, None]
    westward = coeffs[2][offset : offset + extent][:, None]
    middle = fields[1:-1]
    return (
        centre * middle
        + (eastward * fields)[:-2]
        + (westward * fields)[2:]
        + from_south(northward * middle)
        + from_north(southward * middle)
    )


def run_tangent(fields, coeffs, margin):
    for _ in range(STEPS // margin):
        grown = extended(fields, (("tiles", 0),), margin)
        for _ in range(margin):
            offset = (coeffs[0].shape[0] - grown.shape[0]) // 2
            grown = tangent_step(grown, coeffs, offset)
        fields = grown
    return fields


def run_adjoint(fields, coeffs, margin):
    for _ in range(STEPS // margin):
        grown = extended(fields, (("tiles", 0),), margin)
        for _ in range(margin):
            offset = (coeffs[0].shape[0] - grown.shape[0]) // 2
            grown = adjoint_step(grown, coeffs, offset)
        fields = grown
    return fields


def square_tables(extent):
    index = jnp.arange(extent, dtype=jnp.int32)
    phases = index[:, None] * index[None, :] % extent
    angles = phases.astype(jnp.float32) * (2.0 * math.pi / extent)
    return (jnp.cos(angles), jnp.sin(angles))


def contract(form, first, second):
    return jnp.einsum(form, first, second, precision=lax.Precision.HIGHEST)


def smooth_bands(bands, length_sq):
    count = bands.shape[0]
    inner = LON_DEV
    outer = count // inner
    columns = bands.reshape(outer, inner, -1)
    cos_outer, sin_outer = square_tables(outer)
    cos_inner, sin_inner = square_tables(inner)
    outer_index = jnp.arange(outer, dtype=jnp.int32)
    inner_index = jnp.arange(inner, dtype=jnp.int32)
    twist = (outer_index[:, None] * inner_index[None, :] % count).astype(jnp.float32) * (
        2.0 * math.pi / count
    )
    twist_cos = jnp.cos(twist)[:, :, None]
    twist_sin = jnp.sin(twist)[:, :, None]
    first_real = contract("ab,bqc->aqc", cos_outer, columns)
    first_imag = -contract("ab,bqc->aqc", sin_outer, columns)
    turned_real = first_real * twist_cos + first_imag * twist_sin
    turned_imag = first_imag * twist_cos - first_real * twist_sin
    modes_real = contract("aqc,kq->akc", turned_real, cos_inner) + contract(
        "aqc,kq->akc", turned_imag, sin_inner
    )
    modes_imag = contract("aqc,kq->akc", turned_imag, cos_inner) - contract(
        "aqc,kq->akc", turned_real, sin_inner
    )
    wave = (outer_index[:, None] + outer * inner_index[None, :]).astype(jnp.float32)
    basic = 1.0 - jnp.cos(wave * (2.0 * math.pi / count))
    damping = (1.0 + 2.0 * length_sq[None, None, :, None, :] * basic[:, :, None, None, None]) ** (
        -SWEEPS
    )
    damping = jnp.broadcast_to(damping, (outer, inner) + bands.shape[1:]).reshape(outer, inner, -1)
    modes_real = modes_real * damping
    modes_imag = modes_imag * damping
    back_real = contract("akc,kq->aqc", modes_real, cos_inner) - contract(
        "akc,kq->aqc", modes_imag, sin_inner
    )
    back_imag = contract("akc,kq->aqc", modes_imag, cos_inner) + contract(
        "akc,kq->aqc", modes_real, sin_inner
    )
    final_real = back_real * twist_cos - back_imag * twist_sin
    final_imag = back_imag * twist_cos + back_real * twist_sin
    smoothed = contract("ab,bqc->aqc", cos_outer, final_real) - contract(
        "ab,bqc->aqc", sin_outer, final_imag
    )
    return (smoothed / count).reshape(bands.shape)


def body(increment, dual_vector, wind_u, wind_v, land_sea, length_sq, spread):
    margin = 4
    mixing = 0.15 + 0.09 * land_sea.astype(jnp.float32)
    grown_u, grown_v, grown_mix = (
        extended(wind_u, (("tiles", 0),), margin),
        extended(wind_v, (("tiles", 0),), margin),
        extended(mixing, (("tiles", 0),), margin),
    )
    coeffs = coefficients(grown_u, grown_v, grown_mix[:, None, :])
    carried = passed_along(increment[:, -1:], "subwin", 1)
    previous = jnp.concatenate([carried, increment[:, :-1]], axis=1)
    later = passed_along(dual_vector[:, :1], "subwin", -1)
    following = jnp.concatenate([dual_vector[:, 1:], later], axis=1)
    weighted = dual_vector * spread[None, :, :, None]
    bands = lax.all_to_all(weighted, "tiles", split_axis=3, concat_axis=0, tiled=True)
    smoothed = smooth_bands(bands, length_sq)
    forward = run_tangent(previous, coeffs, margin)
    backward = run_adjoint(following, coeffs, margin)
    returned = lax.all_to_all(smoothed, "tiles", split_axis=0, concat_axis=3, tiled=True)
    covar = returned * spread[None, :, :, None]
    return (covar + increment - forward, dual_vector - backward)


SUB = 8
LANES = 128
VMEM_BYTES = 4 * 2**20


def dense_fits(mesh, shape):
    lons, wins, levels, lats = shape
    tiles = mesh.shape["tiles"]
    halves = levels // SUB
    return (
        levels % SUB == 0
        and wins * halves * lats == LANES
        and lons * halves * lats == LANES
        and LANES % levels == 0
        and lats % tiles == 0
        and lons * lats + wins * (lats // tiles) <= LANES
        and mesh.shape["subwin"] == 2
        and tiles % 2 == 0
        and tiles // 2 >= 4
        and STEPS <= 2 * lons
    )


def lane_index():
    return lax.broadcasted_iota(jnp.int32, (SUB, LANES), 1)


def picked(values, index):
    return jnp.take_along_axis(values, index, axis=1)


class Rows:
    def __init__(self, lons, tiles, main, peer, left, right, *far):
        self.tiles = tiles
        self.even = lax.axis_index("tiles") % 2 == 0
        full = 2 * lons + 3
        whole = {row - 1: row * SUB for row in range(full)}
        held = {row - 1: row * SUB for row in range(lons + 1)}
        self.places = ({}, {})
        for odd, sign in enumerate((1, -1)):
            self.add(odd, 0, main, whole, 0, 0)
            self.add(odd, sign, peer, whole, 0, 0)
            for offset, refs in ((-2, left), (2, right)):
                self.add(odd, offset, refs[0], whole, 0, 0)
                if len(refs) == 2:
                    self.add(odd, offset + sign, refs[1], whole, 0, 0)
                else:
                    self.add(odd, offset + sign, refs[0], whole, full - 1, SUB // 2)
            for k, ref in enumerate(far):
                self.add(odd, 2 * (k + 2), ref, held, 0, 0)
                self.add(odd, 2 * (k + 2) + sign, ref, held, lons, SUB // 2)

    def add(self, odd, offset, ref, rows, start, misc):
        for row, at in rows.items():
            at = misc if row < 0 else start * SUB + at
            self.places[odd][offset % self.tiles, row] = (ref, at)

    def __call__(self, offset, row):
        key = (offset % self.tiles, row)
        places = [self.places[odd][key] for odd in (0, 1)]
        if row < 0:
            values = [jnp.broadcast_to(ref[at : at + 1, :], (SUB, LANES)) for ref, at in places]
        else:
            values = [ref[at : at + SUB, :] for ref, at in places]
        if places[0][0] is places[1][0] and places[0][1] == places[1][1]:
            return values[0]
        return jnp.where(self.even, values[0], values[1])


def pack_kernel(*refs):
    arrays, main_ref, held, arrived = refs[:6], refs[6], refs[7:13], refs[13]
    copies = [
        pltpu.make_async_copy(source, target, arrived.at[k])
        for k, (source, target) in enumerate(zip(arrays, held))
    ]
    for copy in copies:
        copy.start()
    for copy in copies:
        copy.wait()
    inc_ref, dual_ref, u_ref, v_ref, land_ref, len_ref = held
    lons, wins, levels, lats = inc_ref.shape
    halves = levels // SUB
    own_lats = len_ref.shape[0]

    def put(row, slot, value):
        at = (row + 1) * SUB
        main_ref[at : at + SUB, slot * lats : (slot + 1) * lats] = value

    for i in range(lons):
        for half in range(halves):
            rows = slice(half * SUB, (half + 1) * SUB)
            for s in range(wins):
                put(i, s * halves + half, dual_ref[i, s, rows, :])
                put(lons + i, s * halves + half, inc_ref[i, s, rows, :])
            put(2 * lons, i * halves + half, u_ref[i, rows, :])
            put(2 * lons + 1, i * halves + half, v_ref[i, rows, :])
    main_ref[:SUB, :] = jnp.zeros((SUB, LANES), jnp.float32)
    for i in range(lons):
        mixing = 0.15 + 0.09 * land_ref[i : i + 1, :].astype(jnp.float32)
        main_ref[:SUB, i * lats : (i + 1) * lats] = jnp.broadcast_to(mixing, (SUB, lats))
    for j in range(own_lats):
        at = lons * lats + j * wins
        main_ref[:SUB, at : at + wins] = jnp.broadcast_to(
            len_ref[j : j + 1, :], (SUB, wins)
        )


def north(values):
    return pltpu.roll(values, LANES - 1, 1)


def south(values):
    return pltpu.roll(values, 1, 1)


def model_kernel(geometry, *refs):
    lons, wins, _, lats, tiles = geometry
    near, (forward_ref, backward_ref, edge_ref, coeff_ref) = refs[:-4], refs[-4:]
    group = LANES // wins
    rows = Rows(lons, tiles, near[0], near[1], near[2:4], near[4:5], *near[5:])
    lane = lane_index()
    lat = lane % lats
    forward, backward = [], []
    for r in range(lons + 2 * STEPS):
        offset, i = (r - STEPS) // lons, (r - STEPS) % lons
        spot = i * group + lane % group
        wind_u = 0.5 * picked(rows(offset, 2 * lons), spot)
        wind_v = 0.5 * picked(rows(offset, 2 * lons + 1), spot)
        mixing = picked(rows(offset, -1), i * lats + lat)
        coeff_ref[r, 0] = 1.0 - 4.0 * mixing
        coeff_ref[r, 1] = mixing - wind_u
        coeff_ref[r, 2] = mixing + wind_u
        coeff_ref[r, 3] = jnp.where(lat == lats - 1, 0.0, mixing - wind_v)
        coeff_ref[r, 4] = jnp.where(lat == 0, 0.0, mixing + wind_v)
        forward.append(rows(offset, lons + i))
        backward.append(rows(offset, i))
    for step in range(STEPS):
        ahead, behind = [], []
        for p in range(1, len(forward) - 1):
            r = p + step
            middle = forward[p]
            ahead.append(
                coeff_ref[r, 0] * middle
                + coeff_ref[r, 1] * forward[p + 1]
                + coeff_ref[r, 2] * forward[p - 1]
                + coeff_ref[r, 3] * north(middle)
                + coeff_ref[r, 4] * south(middle)
            )
            middle = backward[p]
            behind.append(
                coeff_ref[r, 0] * middle
                + coeff_ref[r - 1, 1] * backward[p - 1]
                + coeff_ref[r + 1, 2] * backward[p + 1]
                + south(coeff_ref[r, 3] * middle)
                + north(coeff_ref[r, 4] * middle)
            )
        forward, backward = ahead, behind
    first = lax.axis_index("subwin") == 0
    for i in range(lons):
        at = slice(i * SUB, (i + 1) * SUB)
        forward_ref[at, :] = forward[i]
        backward_ref[at, :] = backward[i]
        edge_ref[at, :] = jnp.where(first, forward[i], backward[i])


def unpack(ref, i, value, wins, halves, lats):
    for s in range(wins):
        for half in range(halves):
            at = (s * halves + half) * lats
            ref[i, s, half * SUB : (half + 1) * SUB, :] = value[:, at : at + lats]


def filter_kernel(geometry, *refs):
    lons, wins, levels, lats, tiles = geometry
    group = LANES // wins
    own_lats = lats // tiles
    count = lons * tiles
    near, (spread_ref, covar_ref) = refs[:-2], refs[-2:]
    rows = Rows(lons, tiles, near[0], near[1], near[2:4], near[4:5], *near[5:])
    lane = lane_index()
    tile = lax.axis_index("tiles")

    length = jnp.zeros((SUB, LANES), jnp.float32)
    index = lons * lats + wins * (lane % own_lats) + lane // group
    owner = lane % lats // own_lats
    for offset in range(tiles):
        here = picked(rows(offset, -1), index)
        length = jnp.where(owner == (tile + offset) % tiles, here, length)
    half = count // 2
    damped = []
    for wave in range(half + 1):
        basic = 1.0 - math.cos(2.0 * math.pi * wave / count)
        inverse = 1.0 / (1.0 + (2.0 * basic) * length)
        squared = inverse * inverse
        weight = (1.0 if wave in (0, half) else 2.0) / count
        damped.append(squared * (squared * weight))

    def waves(gap, start):
        total = None
        for wave in range(start, half + 1, 2):
            factor = math.cos(2.0 * math.pi * (wave * gap % count) / count)
            term = damped[wave] if factor == 1.0 else damped[wave] * factor
            total = term if total is None else total + term
        return total

    weights = [None] * (half + 1)
    for gap in range(half // 2 + 1):
        even, odd = waves(gap, 0), waves(gap, 1)
        weights[gap] = even + odd
        weights[half - gap] = even - odd if half % 2 == 0 else None
    for gap in range(half + 1):
        if weights[gap] is None:
            weights[gap] = waves(gap, 0) + waves(gap, 1)

    smooth = [None] * lons
    for offset in range(tiles):
        for j in range(lons):
            value = rows(offset, j)
            for i in range(lons):
                gap = (i - (offset * lons + j)) % count
                term = weights[min(gap, count - gap)] * value
                smooth[i] = term if smooth[i] is None else smooth[i] + term

    level = lax.broadcasted_iota(jnp.int32, (SUB, LANES), 0) + SUB * (lane % group // lats)
    scale = jnp.zeros((SUB, LANES), jnp.float32)
    for s in range(wins):
        row = jnp.concatenate(
            [jnp.broadcast_to(spread_ref[s : s + 1, :], (SUB, levels))] * (LANES // levels), axis=1
        )
        scale = jnp.where(lane // group == s, picked(row, level), scale)
    square = scale * scale
    for i in range(lons):
        covar_ref[i * SUB : (i + 1) * SUB, :] = square * smooth[i]


def finish_kernel(geometry, *refs):
    lons, wins, levels, lats, _ = geometry
    main, forward_ref, backward_ref, swapped_ref, covar_ref = refs[:5]
    outs, held, sent = refs[5:7], refs[7:9], refs[9]
    group = LANES // wins
    lane = lane_index()
    first = lax.axis_index("subwin") == 0
    copies = [pltpu.make_async_copy(held[k], outs[k], sent.at[k]) for k in (0, 1)]
    for i in range(lons):
        at = slice(i * SUB, (i + 1) * SUB)
        edge = jnp.where(first, swapped_ref[at, :], 0.0)
        behind = jnp.where(lane >= group, backward_ref[at, :], edge)
        value = main[(i + 1) * SUB : (i + 2) * SUB, :] - pltpu.roll(behind, LANES - group, 1)
        unpack(held[1], i, value, wins, levels // SUB, lats)
    copies[1].start()
    for i in range(lons):
        at = slice(i * SUB, (i + 1) * SUB)
        edge = jnp.where(first, 0.0, swapped_ref[at, :])
        ahead = jnp.where(lane < LANES - group, forward_ref[at, :], edge)
        increment = main[(lons + i + 1) * SUB : (lons + i + 2) * SUB, :]
        value = covar_ref[at, :] + increment - pltpu.roll(ahead, group, 1)
        unpack(held[0], i, value, wins, levels // SUB, lats)
    copies[0].start()
    for copy in copies:
        copy.wait()


def kernel_call(kernel, inputs, outputs, scratch=(), flops=0, space=pltpu.VMEM):
    vmem = pl.BlockSpec(memory_space=pltpu.VMEM)
    return pl.pallas_call(
        kernel,
        out_shape=outputs,
        in_specs=[vmem] * len(inputs),
        out_specs=(pl.BlockSpec(memory_space=space),) * len(outputs),
        scratch_shapes=list(scratch),
        compiler_params=pltpu.CompilerParams(vmem_limit_bytes=VMEM_BYTES),
        cost_estimate=pl.CostEstimate(flops=flops, bytes_accessed=2**18, transcendentals=0),
    )(*inputs)


def dense_body(increment, dual_vector, wind_u, wind_v, land_sea, length_sq, spread):
    lons, wins, levels, lats = increment.shape
    tiles = lax.axis_size("tiles")
    rings = tiles // 2
    geometry = (lons, wins, levels, lats, tiles)

    def rows(count):
        return jax.ShapeDtypeStruct((count * SUB, LANES), jnp.float32)

    full = jax.ShapeDtypeStruct(increment.shape, jnp.float32)
    arrays = (increment, dual_vector, wind_u, wind_v, land_sea, length_sq.T)
    main = pl.pallas_call(
        pack_kernel,
        out_shape=rows(2 * lons + 3),
        in_specs=[pl.BlockSpec(memory_space=pltpu.HBM)] * len(arrays),
        out_specs=pl.BlockSpec(memory_space=pltpu.VMEM),
        scratch_shapes=[pltpu.VMEM(x.shape, x.dtype) for x in arrays]
        + [pltpu.SemaphoreType.DMA((len(arrays),))],
        compiler_params=pltpu.CompilerParams(vmem_limit_bytes=VMEM_BYTES),
        name="pack",
    )(*[pltpu.with_memory_space_constraint(x, pltpu.HBM) for x in arrays])

    def moved(x, by):
        pairs = [(t, (t // 2 + by) % rings * 2 + t % 2) for t in range(tiles)]
        return lax.ppermute(x, "tiles", pairs)

    peer = lax.ppermute(main, "tiles", [(t, t ^ 1) for t in range(tiles)])
    row = lax.broadcasted_iota(jnp.int32, (SUB, LANES), 0)
    misc = jnp.where(row < SUB // 2, main[:SUB], peer[:SUB])
    held = (lons + 1) * SUB
    pair = jnp.concatenate([misc, main[SUB:], peer[SUB:]])
    left_own = moved(main, 1)
    left_peer = moved(peer, 1)
    left = (left_own, left_peer)
    right = (moved(pair, -1),)
    short = jnp.concatenate([misc, main[SUB:held], peer[SUB:held]])
    far = [moved(short, -d) for d in range(2, rings - 1)]
    near = (main, peer, *left, *right)
    span = lons + 2 * STEPS
    forward, backward, edge = kernel_call(
        functools.partial(model_kernel, geometry),
        near,
        (rows(lons),) * 3,
        [pltpu.VMEM((span, 5, SUB, LANES), jnp.float32)],
        flops=MODEL_FLOPS,
    )
    swapped = lax.ppermute(edge, "subwin", [(0, 1), (1, 0)])
    (covar,) = kernel_call(
        functools.partial(filter_kernel, geometry),
        (*near, *far, spread),
        (rows(lons),),
        flops=MODEL_FLOPS,
    )
    model_side, dual_side = kernel_call(
        functools.partial(finish_kernel, geometry),
        (main, forward, backward, swapped, covar),
        (full, full),
        [pltpu.VMEM(full.shape, full.dtype)] * 2 + [pltpu.SemaphoreType.DMA((2,))],
        flops=MODEL_FLOPS,
        space=pltpu.HBM,
    )
    return model_side, dual_side


def solution(mesh):
    placed = (
        P(("groups", "tiles"), "subwin", None, None),
        P(("groups", "tiles"), "subwin", None, None),
        P("tiles", None, None),
        P("tiles", None, None),
        P("tiles", None),
        P("subwin", "tiles"),
        P("subwin", None),
    )

    def local(*arrays):
        if dense_fits(mesh, arrays[0].shape):
            return dense_body(*arrays)
        return body(*arrays)

    return jax.shard_map(
        local,
        mesh=mesh,
        in_specs=placed,
        out_specs=(
            P(("groups", "tiles"), "subwin", None, None),
            P(("groups", "tiles"), "subwin", None, None),
        ),
        check_vma=False,
    )
```

```python
import functools
import math

import jax
import jax.numpy as jnp
from jax import lax
from jax.experimental import pallas as pl
from jax.experimental.pallas import tpu as pltpu
from jax.sharding import PartitionSpec as P


STEPS = 8
SWEEPS = 4
LON_DEV = 4
MODEL_FLOPS = 10**6


def extended(x, sides, width):
    for axis, dim in sides:
        devices, length = (lax.axis_size(axis), x.shape[dim])
        up = [(i, (i + 1) % devices) for i in range(devices)]
        down = [(j, i) for i, j in up]
        last = lax.slice_in_dim(x, length - width, length, axis=dim)
        leading = lax.slice_in_dim(x, 0, width, axis=dim)
        before = lax.ppermute(last, axis, up)
        after = lax.ppermute(leading, axis, down)
        x = jnp.concatenate([before, x, after], axis=dim)
    return x


def passed_along(x, axis, by):
    devices = lax.axis_size(axis)
    pairs = [(i, i + by) for i in range(devices) if 0 <= i + by < devices]
    return lax.ppermute(x, axis, pairs)


def from_north(values):
    return jnp.concatenate([values[..., 1:], jnp.zeros_like(values[..., :1])], axis=-1)


def from_south(values):
    return jnp.concatenate([jnp.zeros_like(values[..., :1]), values[..., :-1]], axis=-1)


def coefficients(wind_u, wind_v, mixing):
    return (
        1.0 - 4.0 * mixing,
        mixing - 0.5 * wind_u,
        mixing + 0.5 * wind_u,
        mixing - 0.5 * wind_v,
        mixing + 0.5 * wind_v,
    )


def tangent_step(fields, coeffs, offset):
    extent = fields.shape[0]
    centre, eastward, westward, northward, southward = [
        coeff[offset + 1 : offset + extent - 1][:, None] for coeff in coeffs
    ]
    middle = fields[1:-1]
    return (
        centre * middle
        + eastward * fields[2:]
        + westward * fields[:-2]
        + northward * from_north(middle)
        + southward * from_south(middle)
    )


def adjoint_step(fields, coeffs, offset):
    extent = fields.shape[0]
    centre = coeffs[0][offset + 1 : offset + extent - 1][:, None]
    northward = coeffs[3][offset + 1 : offset + extent - 1][:, None]
    southward = coeffs[4][offset + 1 : offset + extent - 1][:, None]
    eastward = coeffs[1][offset : offset + extent][:, None]
    westward = coeffs[2][offset : offset + extent][:, None]
    middle = fields[1:-1]
    return (
        centre * middle
        + (eastward * fields)[:-2]
        + (westward * fields)[2:]
        + from_south(northward * middle)
        + from_north(southward * middle)
    )


def run_tangent(fields, coeffs, margin):
    for _ in range(STEPS // margin):
        grown = extended(fields, (("tiles", 0),), margin)
        for _ in range(margin):
            offset = (coeffs[0].shape[0] - grown.shape[0]) // 2
            grown = tangent_step(grown, coeffs, offset)
        fields = grown
    return fields


def run_adjoint(fields, coeffs, margin):
    for _ in range(STEPS // margin):
        grown = extended(fields, (("tiles", 0),), margin)
        for _ in range(margin):
            offset = (coeffs[0].shape[0] - grown.shape[0]) // 2
            grown = adjoint_step(grown, coeffs, offset)
        fields = grown
    return fields


def square_tables(extent):
    index = jnp.arange(extent, dtype=jnp.int32)
    phases = index[:, None] * index[None, :] % extent
    angles = phases.astype(jnp.float32) * (2.0 * math.pi / extent)
    return (jnp.cos(angles), jnp.sin(angles))


def contract(form, first, second):
    return jnp.einsum(form, first, second, precision=lax.Precision.HIGHEST)


def smooth_bands(bands, length_sq):
    count = bands.shape[0]
    inner = LON_DEV
    outer = count // inner
    columns = bands.reshape(outer, inner, -1)
    cos_outer, sin_outer = square_tables(outer)
    cos_inner, sin_inner = square_tables(inner)
    outer_index = jnp.arange(outer, dtype=jnp.int32)
    inner_index = jnp.arange(inner, dtype=jnp.int32)
    twist = (outer_index[:, None] * inner_index[None, :] % count).astype(jnp.float32) * (
        2.0 * math.pi / count
    )
    twist_cos = jnp.cos(twist)[:, :, None]
    twist_sin = jnp.sin(twist)[:, :, None]
    first_real = contract("ab,bqc->aqc", cos_outer, columns)
    first_imag = -contract("ab,bqc->aqc", sin_outer, columns)
    turned_real = first_real * twist_cos + first_imag * twist_sin
    turned_imag = first_imag * twist_cos - first_real * twist_sin
    modes_real = contract("aqc,kq->akc", turned_real, cos_inner) + contract(
        "aqc,kq->akc", turned_imag, sin_inner
    )
    modes_imag = contract("aqc,kq->akc", turned_imag, cos_inner) - contract(
        "aqc,kq->akc", turned_real, sin_inner
    )
    wave = (outer_index[:, None] + outer * inner_index[None, :]).astype(jnp.float32)
    basic = 1.0 - jnp.cos(wave * (2.0 * math.pi / count))
    damping = (1.0 + 2.0 * length_sq[None, None, :, None, :] * basic[:, :, None, None, None]) ** (
        -SWEEPS
    )
    damping = jnp.broadcast_to(damping, (outer, inner) + bands.shape[1:]).reshape(outer, inner, -1)
    modes_real = modes_real * damping
    modes_imag = modes_imag * damping
    back_real = contract("akc,kq->aqc", modes_real, cos_inner) - contract(
        "akc,kq->aqc", modes_imag, sin_inner
    )
    back_imag = contract("akc,kq->aqc", modes_imag, cos_inner) + contract(
        "akc,kq->aqc", modes_real, sin_inner
    )
    final_real = back_real * twist_cos - back_imag * twist_sin
    final_imag = back_imag * twist_cos + back_real * twist_sin
    smoothed = contract("ab,bqc->aqc", cos_outer, final_real) - contract(
        "ab,bqc->aqc", sin_outer, final_imag
    )
    return (smoothed / count).reshape(bands.shape)


def body(increment, dual_vector, wind_u, wind_v, land_sea, length_sq, spread):
    margin = 4
    mixing = 0.15 + 0.09 * land_sea.astype(jnp.float32)
    grown_u, grown_v, grown_mix = (
        extended(wind_u, (("tiles", 0),), margin),
        extended(wind_v, (("tiles", 0),), margin),
        extended(mixing, (("tiles", 0),), margin),
    )
    coeffs = coefficients(grown_u, grown_v, grown_mix[:, None, :])
    carried = passed_along(increment[:, -1:], "subwin", 1)
    previous = jnp.concatenate([carried, increment[:, :-1]], axis=1)
    later = passed_along(dual_vector[:, :1], "subwin", -1)
    following = jnp.concatenate([dual_vector[:, 1:], later], axis=1)
    weighted = dual_vector * spread[None, :, :, None]
    bands = lax.all_to_all(weighted, "tiles", split_axis=3, concat_axis=0, tiled=True)
    smoothed = smooth_bands(bands, length_sq)
    forward = run_tangent(previous, coeffs, margin)
    backward = run_adjoint(following, coeffs, margin)
    returned = lax.all_to_all(smoothed, "tiles", split_axis=0, concat_axis=3, tiled=True)
    covar = returned * spread[None, :, :, None]
    return (covar + increment - forward, dual_vector - backward)


SUB = 8
LANES = 128
VMEM_BYTES = 4 * 2**20


def dense_fits(mesh, shape):
    lons, wins, levels, lats = shape
    tiles = mesh.shape["tiles"]
    halves = levels // SUB
    return (
        levels % SUB == 0
        and wins * halves * lats == LANES
        and lons * halves * lats == LANES
        and LANES % levels == 0
        and lats % tiles == 0
        and lons * lats + wins * (lats // tiles) <= LANES
        and mesh.shape["subwin"] == 2
        and tiles % 2 == 0
        and tiles // 2 >= 4
        and STEPS <= 2 * lons
    )


def lane_index():
    return lax.broadcasted_iota(jnp.int32, (SUB, LANES), 1)


def picked(values, index):
    return jnp.take_along_axis(values, index, axis=1)


class Rows:
    def __init__(self, lons, tiles, main, peer, left, right, wide, narrow=None, *far):
        self.tiles = tiles
        self.even = lax.axis_index("tiles") % 2 == 0
        whole = {row - 1: row * SUB for row in range(2 * lons + 3)}
        held = {row - 1: row * SUB for row in range(lons + 1)}
        self.places = ({}, {})
        for odd, sign in enumerate((1, -1)):
            self.add(odd, 0, main, whole, 0, 0)
            self.add(odd, sign, peer, whole, 0, 0)
            self.add(odd, -2, left, whole, 0, 0)
            self.add(odd, 2, right, whole, 0, 0)
            self.add(odd, -sign, wide, whole, 0, 0)
            self.add(odd, 3 * sign, narrow, held, 0, 0)
            for k, ref in enumerate(far):
                self.add(odd, 2 * (k + 2), ref, held, 0, 0)
                self.add(odd, 2 * (k + 2) + sign, ref, held, lons, SUB // 2)

    def add(self, odd, offset, ref, rows, start, misc):
        for row, at in rows.items():
            at = misc if row < 0 else start * SUB + at
            self.places[odd][offset % self.tiles, row] = (ref, at)

    def __call__(self, offset, row):
        key = (offset % self.tiles, row)
        places = [self.places[odd][key] for odd in (0, 1)]
        if row < 0:
            values = [jnp.broadcast_to(ref[at : at + 1, :], (SUB, LANES)) for ref, at in places]
        else:
            values = [ref[at : at + SUB, :] for ref, at in places]
        if places[0][0] is places[1][0] and places[0][1] == places[1][1]:
            return values[0]
        return jnp.where(self.even, values[0], values[1])


def pack_kernel(*refs):
    arrays, main_ref, held, arrived = refs[:6], refs[6], refs[7:13], refs[13]
    copies = [
        pltpu.make_async_copy(source, target, arrived.at[k])
        for k, (source, target) in enumerate(zip(arrays, held))
    ]
    for copy in copies:
        copy.start()
    for copy in copies:
        copy.wait()
    inc_ref, dual_ref, u_ref, v_ref, land_ref, len_ref = held
    lons, wins, levels, lats = inc_ref.shape
    halves = levels // SUB
    own_lats = len_ref.shape[0]

    def put(row, slot, value):
        at = (row + 1) * SUB
        main_ref[at : at + SUB, slot * lats : (slot + 1) * lats] = value

    for i in range(lons):
        for half in range(halves):
            rows = slice(half * SUB, (half + 1) * SUB)
            for s in range(wins):
                put(i, s * halves + half, dual_ref[i, s, rows, :])
                put(lons + i, s * halves + half, inc_ref[i, s, rows, :])
            put(2 * lons, i * halves + half, u_ref[i, rows, :])
            put(2 * lons + 1, i * halves + half, v_ref[i, rows, :])
    main_ref[:SUB, :] = jnp.zeros((SUB, LANES), jnp.float32)
    for i in range(lons):
        mixing = 0.15 + 0.09 * land_ref[i : i + 1, :].astype(jnp.float32)
        main_ref[:SUB, i * lats : (i + 1) * lats] = jnp.broadcast_to(mixing, (SUB, lats))
    for j in range(own_lats):
        at = lons * lats + j * wins
        main_ref[:SUB, at : at + wins] = jnp.broadcast_to(
            len_ref[j : j + 1, :], (SUB, wins)
        )


def north(values):
    return pltpu.roll(values, LANES - 1, 1)


def south(values):
    return pltpu.roll(values, 1, 1)


def model_kernel(geometry, *refs):
    lons, wins, _, lats, tiles = geometry
    near, (forward_ref, backward_ref, edge_ref, coeff_ref) = refs[:-4], refs[-4:]
    group = LANES // wins
    rows = Rows(lons, tiles, *near)
    lane = lane_index()
    lat = lane % lats
    forward, backward = [], []
    for r in range(lons + 2 * STEPS):
        offset, i = (r - STEPS) // lons, (r - STEPS) % lons
        spot = i * group + lane % group
        wind_u = 0.5 * picked(rows(offset, 2 * lons), spot)
        wind_v = 0.5 * picked(rows(offset, 2 * lons + 1), spot)
        mixing = picked(rows(offset, -1), i * lats + lat)
        coeff_ref[r, 0] = 1.0 - 4.0 * mixing
        coeff_ref[r, 1] = mixing - wind_u
        coeff_ref[r, 2] = mixing + wind_u
        coeff_ref[r, 3] = jnp.where(lat == lats - 1, 0.0, mixing - wind_v)
        coeff_ref[r, 4] = jnp.where(lat == 0, 0.0, mixing + wind_v)
        forward.append(rows(offset, lons + i))
        backward.append(rows(offset, i))
    for step in range(STEPS):
        ahead, behind = [], []
        for p in range(1, len(forward) - 1):
            r = p + step
            middle = forward[p]
            ahead.append(
                coeff_ref[r, 0] * middle
                + coeff_ref[r, 1] * forward[p + 1]
                + coeff_ref[r, 2] * forward[p - 1]
                + coeff_ref[r, 3] * north(middle)
                + coeff_ref[r, 4] * south(middle)
            )
            middle = backward[p]
            behind.append(
                coeff_ref[r, 0] * middle
                + coeff_ref[r - 1, 1] * backward[p - 1]
                + coeff_ref[r + 1, 2] * backward[p + 1]
                + south(coeff_ref[r, 3] * middle)
                + north(coeff_ref[r, 4] * middle)
            )
        forward, backward = ahead, behind
    first = lax.axis_index("subwin") == 0
    for i in range(lons):
        at = slice(i * SUB, (i + 1) * SUB)
        forward_ref[at, :] = forward[i]
        backward_ref[at, :] = backward[i]
        edge_ref[at, :] = jnp.where(first, forward[i], backward[i])


def unpack(ref, i, value, wins, halves, lats):
    for s in range(wins):
        for half in range(halves):
            at = (s * halves + half) * lats
            ref[i, s, half * SUB : (half + 1) * SUB, :] = value[:, at : at + lats]


def filter_kernel(geometry, *refs):
    lons, wins, levels, lats, tiles = geometry
    group = LANES // wins
    own_lats = lats // tiles
    count = lons * tiles
    spread_ref, covar_ref = refs[-2:]
    rows = Rows(lons, tiles, *refs[:-2])
    lane = lane_index()
    tile = lax.axis_index("tiles")

    length = jnp.zeros((SUB, LANES), jnp.float32)
    index = lons * lats + wins * (lane % own_lats) + lane // group
    owner = lane % lats // own_lats
    for offset in range(tiles):
        here = picked(rows(offset, -1), index)
        length = jnp.where(owner == (tile + offset) % tiles, here, length)
    half = count // 2
    damped = []
    for wave in range(half + 1):
        basic = 1.0 - math.cos(2.0 * math.pi * wave / count)
        inverse = 1.0 / (1.0 + (2.0 * basic) * length)
        squared = inverse * inverse
        weight = (1.0 if wave in (0, half) else 2.0) / count
        damped.append(squared * (squared * weight))

    def waves(gap, start):
        total = None
        for wave in range(start, half + 1, 2):
            factor = math.cos(2.0 * math.pi * (wave * gap % count) / count)
            term = damped[wave] if factor == 1.0 else damped[wave] * factor
            total = term if total is None else total + term
        return total

    weights = [None] * (half + 1)
    for gap in range(half // 2 + 1):
        even, odd = waves(gap, 0), waves(gap, 1)
        weights[gap] = even + odd
        weights[half - gap] = even - odd if half % 2 == 0 else None
    for gap in range(half + 1):
        if weights[gap] is None:
            weights[gap] = waves(gap, 0) + waves(gap, 1)

    smooth = [None] * lons
    for offset in range(tiles):
        for j in range(lons):
            value = rows(offset, j)
            for i in range(lons):
                gap = (i - (offset * lons + j)) % count
                term = weights[min(gap, count - gap)] * value
                smooth[i] = term if smooth[i] is None else smooth[i] + term

    level = lax.broadcasted_iota(jnp.int32, (SUB, LANES), 0) + SUB * (lane % group // lats)
    scale = jnp.zeros((SUB, LANES), jnp.float32)
    for s in range(wins):
        row = jnp.concatenate(
            [jnp.broadcast_to(spread_ref[s : s + 1, :], (SUB, levels))] * (LANES // levels), axis=1
        )
        scale = jnp.where(lane // group == s, picked(row, level), scale)
    square = scale * scale
    for i in range(lons):
        covar_ref[i * SUB : (i + 1) * SUB, :] = square * smooth[i]


def finish_kernel(geometry, *refs):
    lons, wins, levels, lats, _ = geometry
    main, forward_ref, backward_ref, swapped_ref, covar_ref = refs[:5]
    outs, held, sent = refs[5:7], refs[7:9], refs[9]
    group = LANES // wins
    lane = lane_index()
    first = lax.axis_index("subwin") == 0
    copies = [pltpu.make_async_copy(held[k], outs[k], sent.at[k]) for k in (0, 1)]
    for i in range(lons):
        at = slice(i * SUB, (i + 1) * SUB)
        edge = jnp.where(first, swapped_ref[at, :], 0.0)
        behind = jnp.where(lane >= group, backward_ref[at, :], edge)
        value = main[(i + 1) * SUB : (i + 2) * SUB, :] - pltpu.roll(behind, LANES - group, 1)
        unpack(held[1], i, value, wins, levels // SUB, lats)
    copies[1].start()
    for i in range(lons):
        at = slice(i * SUB, (i + 1) * SUB)
        edge = jnp.where(first, 0.0, swapped_ref[at, :])
        ahead = jnp.where(lane < LANES - group, forward_ref[at, :], edge)
        increment = main[(lons + i + 1) * SUB : (lons + i + 2) * SUB, :]
        value = covar_ref[at, :] + increment - pltpu.roll(ahead, group, 1)
        unpack(held[0], i, value, wins, levels // SUB, lats)
    copies[0].start()
    for copy in copies:
        copy.wait()


def kernel_call(kernel, inputs, outputs, scratch=(), flops=0, space=pltpu.VMEM):
    vmem = pl.BlockSpec(memory_space=pltpu.VMEM)
    return pl.pallas_call(
        kernel,
        out_shape=outputs,
        in_specs=[vmem] * len(inputs),
        out_specs=(pl.BlockSpec(memory_space=space),) * len(outputs),
        scratch_shapes=list(scratch),
        compiler_params=pltpu.CompilerParams(vmem_limit_bytes=VMEM_BYTES),
        cost_estimate=pl.CostEstimate(flops=flops, bytes_accessed=2**18, transcendentals=0),
    )(*inputs)


def dense_body(increment, dual_vector, wind_u, wind_v, land_sea, length_sq, spread):
    lons, wins, levels, lats = increment.shape
    tiles = lax.axis_size("tiles")
    rings = tiles // 2
    geometry = (lons, wins, levels, lats, tiles)

    def rows(count):
        return jax.ShapeDtypeStruct((count * SUB, LANES), jnp.float32)

    full = jax.ShapeDtypeStruct(increment.shape, jnp.float32)
    arrays = (increment, dual_vector, wind_u, wind_v, land_sea, length_sq.T)
    main = pl.pallas_call(
        pack_kernel,
        out_shape=rows(2 * lons + 3),
        in_specs=[pl.BlockSpec(memory_space=pltpu.HBM)] * len(arrays),
        out_specs=pl.BlockSpec(memory_space=pltpu.VMEM),
        scratch_shapes=[pltpu.VMEM(x.shape, x.dtype) for x in arrays]
        + [pltpu.SemaphoreType.DMA((len(arrays),))],
        compiler_params=pltpu.CompilerParams(vmem_limit_bytes=VMEM_BYTES),
        name="pack",
    )(*[pltpu.with_memory_space_constraint(x, pltpu.HBM) for x in arrays])

    def moved(x, by):
        pairs = [(t, (t // 2 + by(t % 2)) % rings * 2 + t % 2) for t in range(tiles)]
        return lax.ppermute(x, "tiles", pairs)

    peer = lax.ppermute(main, "tiles", [(t, t ^ 1) for t in range(tiles)])
    row = lax.broadcasted_iota(jnp.int32, (SUB, LANES), 0)
    misc = jnp.where(row < SUB // 2, main[:SUB], peer[:SUB])
    held = (lons + 1) * SUB
    left = moved(main, lambda odd: 1)
    right = moved(main, lambda odd: -1)
    wide = lax.ppermute(
        main,
        "tiles",
        [(t, (t + 1 if t % 2 else t - 1) % tiles) for t in range(tiles)],
    )
    narrow = moved(peer[:held], lambda odd: 1 if odd else -1)
    short = jnp.concatenate([misc, main[SUB:held], peer[SUB:held]])
    far = [moved(short, lambda odd, d=d: -d) for d in range(2, rings - 1)]
    near = (main, peer, left, right, wide)
    span = lons + 2 * STEPS
    forward, backward, edge = kernel_call(
        functools.partial(model_kernel, geometry),
        near,
        (rows(lons),) * 3,
        [pltpu.VMEM((span, 5, SUB, LANES), jnp.float32)],
        flops=MODEL_FLOPS,
    )
    swapped = lax.ppermute(edge, "subwin", [(0, 1), (1, 0)])
    (covar,) = kernel_call(
        functools.partial(filter_kernel, geometry),
        (*near, narrow, *far, spread),
        (rows(lons),),
        flops=MODEL_FLOPS,
    )
    model_side, dual_side = kernel_call(
        functools.partial(finish_kernel, geometry),
        (main, forward, backward, swapped, covar),
        (full, full),
        [pltpu.VMEM(full.shape, full.dtype)] * 2 + [pltpu.SemaphoreType.DMA((2,))],
        flops=MODEL_FLOPS,
        space=pltpu.HBM,
    )
    return model_side, dual_side


def solution(mesh):
    placed = (
        P(("groups", "tiles"), "subwin", None, None),
        P(("groups", "tiles"), "subwin", None, None),
        P("tiles", None, None),
        P("tiles", None, None),
        P("tiles", None),
        P("subwin", "tiles"),
        P("subwin", None),
    )

    def local(*arrays):
        if dense_fits(mesh, arrays[0].shape):
            return dense_body(*arrays)
        return body(*arrays)

    return jax.shard_map(
        local,
        mesh=mesh,
        in_specs=placed,
        out_specs=(
            P(("groups", "tiles"), "subwin", None, None),
            P(("groups", "tiles"), "subwin", None, None),
        ),
        check_vma=False,
    )
```

```python
import functools
import math

import jax
import jax.numpy as jnp
from jax import lax
from jax.experimental import pallas as pl
from jax.experimental.pallas import tpu as pltpu
from jax.sharding import PartitionSpec as P


STEPS = 8
SWEEPS = 4
LON_DEV = 4
MODEL_FLOPS = 10**6


def extended(x, sides, width):
    for axis, dim in sides:
        devices, length = (lax.axis_size(axis), x.shape[dim])
        up = [(i, (i + 1) % devices) for i in range(devices)]
        down = [(j, i) for i, j in up]
        last = lax.slice_in_dim(x, length - width, length, axis=dim)
        leading = lax.slice_in_dim(x, 0, width, axis=dim)
        before = lax.ppermute(last, axis, up)
        after = lax.ppermute(leading, axis, down)
        x = jnp.concatenate([before, x, after], axis=dim)
    return x


def passed_along(x, axis, by):
    devices = lax.axis_size(axis)
    pairs = [(i, i + by) for i in range(devices) if 0 <= i + by < devices]
    return lax.ppermute(x, axis, pairs)


def from_north(values):
    return jnp.concatenate([values[..., 1:], jnp.zeros_like(values[..., :1])], axis=-1)


def from_south(values):
    return jnp.concatenate([jnp.zeros_like(values[..., :1]), values[..., :-1]], axis=-1)


def coefficients(wind_u, wind_v, mixing):
    return (
        1.0 - 4.0 * mixing,
        mixing - 0.5 * wind_u,
        mixing + 0.5 * wind_u,
        mixing - 0.5 * wind_v,
        mixing + 0.5 * wind_v,
    )


def tangent_step(fields, coeffs, offset):
    extent = fields.shape[0]
    centre, eastward, westward, northward, southward = [
        coeff[offset + 1 : offset + extent - 1][:, None] for coeff in coeffs
    ]
    middle = fields[1:-1]
    return (
        centre * middle
        + eastward * fields[2:]
        + westward * fields[:-2]
        + northward * from_north(middle)
        + southward * from_south(middle)
    )


def adjoint_step(fields, coeffs, offset):
    extent = fields.shape[0]
    centre = coeffs[0][offset + 1 : offset + extent - 1][:, None]
    northward = coeffs[3][offset + 1 : offset + extent - 1][:, None]
    southward = coeffs[4][offset + 1 : offset + extent - 1][:, None]
    eastward = coeffs[1][offset : offset + extent][:, None]
    westward = coeffs[2][offset : offset + extent][:, None]
    middle = fields[1:-1]
    return (
        centre * middle
        + (eastward * fields)[:-2]
        + (westward * fields)[2:]
        + from_south(northward * middle)
        + from_north(southward * middle)
    )


def run_tangent(fields, coeffs, margin):
    for _ in range(STEPS // margin):
        grown = extended(fields, (("tiles", 0),), margin)
        for _ in range(margin):
            offset = (coeffs[0].shape[0] - grown.shape[0]) // 2
            grown = tangent_step(grown, coeffs, offset)
        fields = grown
    return fields


def run_adjoint(fields, coeffs, margin):
    for _ in range(STEPS // margin):
        grown = extended(fields, (("tiles", 0),), margin)
        for _ in range(margin):
            offset = (coeffs[0].shape[0] - grown.shape[0]) // 2
            grown = adjoint_step(grown, coeffs, offset)
        fields = grown
    return fields


def square_tables(extent):
    index = jnp.arange(extent, dtype=jnp.int32)
    phases = index[:, None] * index[None, :] % extent
    angles = phases.astype(jnp.float32) * (2.0 * math.pi / extent)
    return (jnp.cos(angles), jnp.sin(angles))


def contract(form, first, second):
    return jnp.einsum(form, first, second, precision=lax.Precision.HIGHEST)


def smooth_bands(bands, length_sq):
    count = bands.shape[0]
    inner = LON_DEV
    outer = count // inner
    columns = bands.reshape(outer, inner, -1)
    cos_outer, sin_outer = square_tables(outer)
    cos_inner, sin_inner = square_tables(inner)
    outer_index = jnp.arange(outer, dtype=jnp.int32)
    inner_index = jnp.arange(inner, dtype=jnp.int32)
    twist = (outer_index[:, None] * inner_index[None, :] % count).astype(jnp.float32) * (
        2.0 * math.pi / count
    )
    twist_cos = jnp.cos(twist)[:, :, None]
    twist_sin = jnp.sin(twist)[:, :, None]
    first_real = contract("ab,bqc->aqc", cos_outer, columns)
    first_imag = -contract("ab,bqc->aqc", sin_outer, columns)
    turned_real = first_real * twist_cos + first_imag * twist_sin
    turned_imag = first_imag * twist_cos - first_real * twist_sin
    modes_real = contract("aqc,kq->akc", turned_real, cos_inner) + contract(
        "aqc,kq->akc", turned_imag, sin_inner
    )
    modes_imag = contract("aqc,kq->akc", turned_imag, cos_inner) - contract(
        "aqc,kq->akc", turned_real, sin_inner
    )
    wave = (outer_index[:, None] + outer * inner_index[None, :]).astype(jnp.float32)
    basic = 1.0 - jnp.cos(wave * (2.0 * math.pi / count))
    damping = (1.0 + 2.0 * length_sq[None, None, :, None, :] * basic[:, :, None, None, None]) ** (
        -SWEEPS
    )
    damping = jnp.broadcast_to(damping, (outer, inner) + bands.shape[1:]).reshape(outer, inner, -1)
    modes_real = modes_real * damping
    modes_imag = modes_imag * damping
    back_real = contract("akc,kq->aqc", modes_real, cos_inner) - contract(
        "akc,kq->aqc", modes_imag, sin_inner
    )
    back_imag = contract("akc,kq->aqc", modes_imag, cos_inner) + contract(
        "akc,kq->aqc", modes_real, sin_inner
    )
    final_real = back_real * twist_cos - back_imag * twist_sin
    final_imag = back_imag * twist_cos + back_real * twist_sin
    smoothed = contract("ab,bqc->aqc", cos_outer, final_real) - contract(
        "ab,bqc->aqc", sin_outer, final_imag
    )
    return (smoothed / count).reshape(bands.shape)


def body(increment, dual_vector, wind_u, wind_v, land_sea, length_sq, spread):
    margin = 4
    mixing = 0.15 + 0.09 * land_sea.astype(jnp.float32)
    grown_u, grown_v, grown_mix = (
        extended(wind_u, (("tiles", 0),), margin),
        extended(wind_v, (("tiles", 0),), margin),
        extended(mixing, (("tiles", 0),), margin),
    )
    coeffs = coefficients(grown_u, grown_v, grown_mix[:, None, :])
    carried = passed_along(increment[:, -1:], "subwin", 1)
    previous = jnp.concatenate([carried, increment[:, :-1]], axis=1)
    later = passed_along(dual_vector[:, :1], "subwin", -1)
    following = jnp.concatenate([dual_vector[:, 1:], later], axis=1)
    weighted = dual_vector * spread[None, :, :, None]
    bands = lax.all_to_all(weighted, "tiles", split_axis=3, concat_axis=0, tiled=True)
    smoothed = smooth_bands(bands, length_sq)
    forward = run_tangent(previous, coeffs, margin)
    backward = run_adjoint(following, coeffs, margin)
    returned = lax.all_to_all(smoothed, "tiles", split_axis=0, concat_axis=3, tiled=True)
    covar = returned * spread[None, :, :, None]
    return (covar + increment - forward, dual_vector - backward)


SUB = 8
LANES = 128
VMEM_BYTES = 4 * 2**20


def dense_fits(mesh, shape):
    lons, wins, levels, lats = shape
    tiles = mesh.shape["tiles"]
    halves = levels // SUB
    return (
        levels % SUB == 0
        and wins * halves * lats == LANES
        and lons * halves * lats == LANES
        and LANES % levels == 0
        and lats % tiles == 0
        and lons * lats + wins * (lats // tiles) <= LANES
        and mesh.shape["subwin"] == 2
        and tiles % 2 == 0
        and tiles // 2 >= 4
        and STEPS <= 2 * lons
    )


def lane_index():
    return lax.broadcasted_iota(jnp.int32, (SUB, LANES), 1)


def picked(values, index):
    return jnp.take_along_axis(values, index, axis=1)


class Rows:
    def __init__(self, lons, tiles, main, peer, left, right, wide, narrow=None, *far):
        self.tiles = tiles
        self.even = lax.axis_index("tiles") % 2 == 0
        whole = {row - 1: row * SUB for row in range(2 * lons + 3)}
        held = {row - 1: row * SUB for row in range(lons + 1)}
        self.places = ({}, {})
        for odd, sign in enumerate((1, -1)):
            self.add(odd, 0, main, whole, 0, 0)
            self.add(odd, sign, peer, whole, 0, 0)
            self.add(odd, -2, left, whole, 0, 0)
            self.add(odd, 2, right, whole, 0, 0)
            self.add(odd, -sign, wide, whole, 0, 0)
            self.add(odd, 3 * sign, narrow, held, 0, 0)
            for k, ref in enumerate(far):
                self.add(odd, 2 * (k + 2), ref, held, 0, 0)
                self.add(odd, 2 * (k + 2) + sign, ref, held, lons, SUB // 2)

    def add(self, odd, offset, ref, rows, start, misc):
        for row, at in rows.items():
            at = misc if row < 0 else start * SUB + at
            self.places[odd][offset % self.tiles, row] = (ref, at)

    def __call__(self, offset, row):
        key = (offset % self.tiles, row)
        places = [self.places[odd][key] for odd in (0, 1)]
        if row < 0:
            values = [jnp.broadcast_to(ref[at : at + 1, :], (SUB, LANES)) for ref, at in places]
        else:
            values = [ref[at : at + SUB, :] for ref, at in places]
        if places[0][0] is places[1][0] and places[0][1] == places[1][1]:
            return values[0]
        return jnp.where(self.even, values[0], values[1])


def pack_kernel(*refs):
    arrays, main_ref, held, arrived = refs[:6], refs[6], refs[7:13], refs[13]
    copies = [
        pltpu.make_async_copy(source, target, arrived.at[k])
        for k, (source, target) in enumerate(zip(arrays, held))
    ]
    for copy in copies:
        copy.start()
    for copy in copies:
        copy.wait()
    inc_ref, dual_ref, u_ref, v_ref, land_ref, len_ref = held
    lons, wins, levels, lats = inc_ref.shape
    halves = levels // SUB
    own_lats = len_ref.shape[0]

    def put(row, slot, value):
        at = (row + 1) * SUB
        main_ref[at : at + SUB, slot * lats : (slot + 1) * lats] = value

    for i in range(lons):
        for half in range(halves):
            rows = slice(half * SUB, (half + 1) * SUB)
            for s in range(wins):
                put(i, s * halves + half, dual_ref[i, s, rows, :])
                put(lons + i, s * halves + half, inc_ref[i, s, rows, :])
            put(2 * lons, i * halves + half, u_ref[i, rows, :])
            put(2 * lons + 1, i * halves + half, v_ref[i, rows, :])
    main_ref[:SUB, :] = jnp.zeros((SUB, LANES), jnp.float32)
    for i in range(lons):
        mixing = 0.15 + 0.09 * land_ref[i : i + 1, :].astype(jnp.float32)
        main_ref[:SUB, i * lats : (i + 1) * lats] = jnp.broadcast_to(mixing, (SUB, lats))
    for j in range(own_lats):
        at = lons * lats + j * wins
        main_ref[:SUB, at : at + wins] = jnp.broadcast_to(
            len_ref[j : j + 1, :], (SUB, wins)
        )


def north(values):
    return pltpu.roll(values, LANES - 1, 1)


def south(values):
    return pltpu.roll(values, 1, 1)


def model_kernel(geometry, *refs):
    lons, wins, _, lats, tiles = geometry
    near, (forward_ref, backward_ref, edge_ref, coeff_ref) = refs[:-4], refs[-4:]
    group = LANES // wins
    rows = Rows(lons, tiles, *near)
    lane = lane_index()
    lat = lane % lats
    forward, backward = [], []
    for r in range(lons + 2 * STEPS):
        offset, i = (r - STEPS) // lons, (r - STEPS) % lons
        spot = i * group + lane % group
        wind_u = 0.5 * picked(rows(offset, 2 * lons), spot)
        wind_v = 0.5 * picked(rows(offset, 2 * lons + 1), spot)
        mixing = picked(rows(offset, -1), i * lats + lat)
        coeff_ref[r, 0] = 1.0 - 4.0 * mixing
        coeff_ref[r, 1] = mixing - wind_u
        coeff_ref[r, 2] = mixing + wind_u
        coeff_ref[r, 3] = jnp.where(lat == lats - 1, 0.0, mixing - wind_v)
        coeff_ref[r, 4] = jnp.where(lat == 0, 0.0, mixing + wind_v)
        forward.append(rows(offset, lons + i))
        backward.append(rows(offset, i))
    for step in range(STEPS):
        ahead, behind = [], []
        for p in range(1, len(forward) - 1):
            r = p + step
            middle = forward[p]
            ahead.append(
                coeff_ref[r, 0] * middle
                + coeff_ref[r, 1] * forward[p + 1]
                + coeff_ref[r, 2] * forward[p - 1]
                + coeff_ref[r, 3] * north(middle)
                + coeff_ref[r, 4] * south(middle)
            )
            middle = backward[p]
            behind.append(
                coeff_ref[r, 0] * middle
                + coeff_ref[r - 1, 1] * backward[p - 1]
                + coeff_ref[r + 1, 2] * backward[p + 1]
                + south(coeff_ref[r, 3] * middle)
                + north(coeff_ref[r, 4] * middle)
            )
        forward, backward = ahead, behind
    first = lax.axis_index("subwin") == 0
    for i in range(lons):
        at = slice(i * SUB, (i + 1) * SUB)
        forward_ref[at, :] = forward[i]
        backward_ref[at, :] = backward[i]
        edge_ref[at, :] = jnp.where(first, forward[i], backward[i])


def unpack(ref, i, value, wins, halves, lats):
    for s in range(wins):
        for half in range(halves):
            at = (s * halves + half) * lats
            ref[i, s, half * SUB : (half + 1) * SUB, :] = value[:, at : at + lats]


def filtered(geometry, spread_ref, *refs):
    lons, wins, levels, lats, tiles = geometry
    group = LANES // wins
    own_lats = lats // tiles
    count = lons * tiles
    rows = Rows(lons, tiles, *refs)
    lane = lane_index()
    tile = lax.axis_index("tiles")

    length = jnp.zeros((SUB, LANES), jnp.float32)
    index = lons * lats + wins * (lane % own_lats) + lane // group
    owner = lane % lats // own_lats
    for offset in range(tiles):
        here = picked(rows(offset, -1), index)
        length = jnp.where(owner == (tile + offset) % tiles, here, length)
    half = count // 2
    damped = []
    for wave in range(half + 1):
        basic = 1.0 - math.cos(2.0 * math.pi * wave / count)
        inverse = 1.0 / (1.0 + (2.0 * basic) * length)
        squared = inverse * inverse
        weight = (1.0 if wave in (0, half) else 2.0) / count
        damped.append(squared * (squared * weight))

    def waves(gap, start):
        total = None
        for wave in range(start, half + 1, 2):
            factor = math.cos(2.0 * math.pi * (wave * gap % count) / count)
            term = damped[wave] if factor == 1.0 else damped[wave] * factor
            total = term if total is None else total + term
        return total

    weights = [None] * (half + 1)
    for gap in range(half // 2 + 1):
        even, odd = waves(gap, 0), waves(gap, 1)
        weights[gap] = even + odd
        weights[half - gap] = even - odd if half % 2 == 0 else None
    for gap in range(half + 1):
        if weights[gap] is None:
            weights[gap] = waves(gap, 0) + waves(gap, 1)

    smooth = [None] * lons
    for offset in range(tiles):
        for j in range(lons):
            value = rows(offset, j)
            for i in range(lons):
                gap = (i - (offset * lons + j)) % count
                term = weights[min(gap, count - gap)] * value
                smooth[i] = term if smooth[i] is None else smooth[i] + term

    level = lax.broadcasted_iota(jnp.int32, (SUB, LANES), 0) + SUB * (lane % group // lats)
    scale = jnp.zeros((SUB, LANES), jnp.float32)
    for s in range(wins):
        row = jnp.concatenate(
            [jnp.broadcast_to(spread_ref[s : s + 1, :], (SUB, levels))] * (LANES // levels), axis=1
        )
        scale = jnp.where(lane // group == s, picked(row, level), scale)
    square = scale * scale
    for i in range(lons):
        smooth[i] = square * smooth[i]
    return smooth


def finish_kernel(geometry, *refs):
    lons, wins, levels, lats, _ = geometry
    main, forward_ref, backward_ref, swapped_ref, spread_ref = refs[0], *refs[-9:-5]
    outs, held, sent = refs[-5:-3], refs[-3:-1], refs[-1]
    group = LANES // wins
    lane = lane_index()
    first = lax.axis_index("subwin") == 0
    copies = [pltpu.make_async_copy(held[k], outs[k], sent.at[k]) for k in (0, 1)]
    for i in range(lons):
        at = slice(i * SUB, (i + 1) * SUB)
        edge = jnp.where(first, swapped_ref[at, :], 0.0)
        behind = jnp.where(lane >= group, backward_ref[at, :], edge)
        value = main[(i + 1) * SUB : (i + 2) * SUB, :] - pltpu.roll(behind, LANES - group, 1)
        unpack(held[1], i, value, wins, levels // SUB, lats)
    copies[1].start()
    covar = filtered(geometry, spread_ref, *refs[:-9])
    for i in range(lons):
        at = slice(i * SUB, (i + 1) * SUB)
        edge = jnp.where(first, 0.0, swapped_ref[at, :])
        ahead = jnp.where(lane < LANES - group, forward_ref[at, :], edge)
        increment = main[(lons + i + 1) * SUB : (lons + i + 2) * SUB, :]
        value = covar[i] + increment - pltpu.roll(ahead, group, 1)
        unpack(held[0], i, value, wins, levels // SUB, lats)
    copies[0].start()
    for copy in copies:
        copy.wait()


def kernel_call(kernel, inputs, outputs, scratch=(), flops=0, space=pltpu.VMEM):
    vmem = pl.BlockSpec(memory_space=pltpu.VMEM)
    return pl.pallas_call(
        kernel,
        out_shape=outputs,
        in_specs=[vmem] * len(inputs),
        out_specs=(pl.BlockSpec(memory_space=space),) * len(outputs),
        scratch_shapes=list(scratch),
        compiler_params=pltpu.CompilerParams(vmem_limit_bytes=VMEM_BYTES),
        cost_estimate=pl.CostEstimate(flops=flops, bytes_accessed=2**18, transcendentals=0),
    )(*inputs)


def dense_body(increment, dual_vector, wind_u, wind_v, land_sea, length_sq, spread):
    lons, wins, levels, lats = increment.shape
    tiles = lax.axis_size("tiles")
    rings = tiles // 2
    geometry = (lons, wins, levels, lats, tiles)

    def rows(count):
        return jax.ShapeDtypeStruct((count * SUB, LANES), jnp.float32)

    full = jax.ShapeDtypeStruct(increment.shape, jnp.float32)
    arrays = (increment, dual_vector, wind_u, wind_v, land_sea, length_sq.T)
    main = pl.pallas_call(
        pack_kernel,
        out_shape=rows(2 * lons + 3),
        in_specs=[pl.BlockSpec(memory_space=pltpu.HBM)] * len(arrays),
        out_specs=pl.BlockSpec(memory_space=pltpu.VMEM),
        scratch_shapes=[pltpu.VMEM(x.shape, x.dtype) for x in arrays]
        + [pltpu.SemaphoreType.DMA((len(arrays),))],
        compiler_params=pltpu.CompilerParams(vmem_limit_bytes=VMEM_BYTES),
        name="pack",
    )(*[pltpu.with_memory_space_constraint(x, pltpu.HBM) for x in arrays])

    def moved(x, by):
        pairs = [(t, (t // 2 + by(t % 2)) % rings * 2 + t % 2) for t in range(tiles)]
        return lax.ppermute(x, "tiles", pairs)

    peer = lax.ppermute(main, "tiles", [(t, t ^ 1) for t in range(tiles)])
    row = lax.broadcasted_iota(jnp.int32, (SUB, LANES), 0)
    misc = jnp.where(row < SUB // 2, main[:SUB], peer[:SUB])
    held = (lons + 1) * SUB
    left = moved(main, lambda odd: 1)
    right = moved(main, lambda odd: -1)
    wide = lax.ppermute(
        main,
        "tiles",
        [(t, (t + 1 if t % 2 else t - 1) % tiles) for t in range(tiles)],
    )
    narrow = moved(peer[:held], lambda odd: 1 if odd else -1)
    short = jnp.concatenate([misc, main[SUB:held], peer[SUB:held]])
    far = [moved(short, lambda odd, d=d: -d) for d in range(2, rings - 1)]
    near = (main, peer, left, right, wide)
    span = lons + 2 * STEPS
    forward, backward, edge = kernel_call(
        functools.partial(model_kernel, geometry),
        near,
        (rows(lons),) * 3,
        [pltpu.VMEM((span, 5, SUB, LANES), jnp.float32)],
        flops=MODEL_FLOPS,
    )
    swapped = lax.ppermute(edge, "subwin", [(0, 1), (1, 0)])
    model_side, dual_side = kernel_call(
        functools.partial(finish_kernel, geometry),
        (*near, narrow, *far, forward, backward, swapped, spread),
        (full, full),
        [pltpu.VMEM(full.shape, full.dtype)] * 2 + [pltpu.SemaphoreType.DMA((2,))],
        flops=MODEL_FLOPS,
        space=pltpu.HBM,
    )
    return model_side, dual_side


def solution(mesh):
    placed = (
        P(("groups", "tiles"), "subwin", None, None),
        P(("groups", "tiles"), "subwin", None, None),
        P("tiles", None, None),
        P("tiles", None, None),
        P("tiles", None),
        P("subwin", "tiles"),
        P("subwin", None),
    )

    def local(*arrays):
        if dense_fits(mesh, arrays[0].shape):
            return dense_body(*arrays)
        return body(*arrays)

    return jax.shard_map(
        local,
        mesh=mesh,
        in_specs=placed,
        out_specs=(
            P(("groups", "tiles"), "subwin", None, None),
            P(("groups", "tiles"), "subwin", None, None),
        ),
        check_vma=False,
    )
```

```python
import functools
import math

import jax
import jax.numpy as jnp
from jax import lax
from jax.experimental import pallas as pl
from jax.experimental.pallas import tpu as pltpu
from jax.sharding import PartitionSpec as P


STEPS = 8
SWEEPS = 4
LON_DEV = 4
MODEL_FLOPS = 10**6


def extended(x, sides, width):
    for axis, dim in sides:
        devices, length = (lax.axis_size(axis), x.shape[dim])
        up = [(i, (i + 1) % devices) for i in range(devices)]
        down = [(j, i) for i, j in up]
        last = lax.slice_in_dim(x, length - width, length, axis=dim)
        leading = lax.slice_in_dim(x, 0, width, axis=dim)
        before = lax.ppermute(last, axis, up)
        after = lax.ppermute(leading, axis, down)
        x = jnp.concatenate([before, x, after], axis=dim)
    return x


def passed_along(x, axis, by):
    devices = lax.axis_size(axis)
    pairs = [(i, i + by) for i in range(devices) if 0 <= i + by < devices]
    return lax.ppermute(x, axis, pairs)


def from_north(values):
    return jnp.concatenate([values[..., 1:], jnp.zeros_like(values[..., :1])], axis=-1)


def from_south(values):
    return jnp.concatenate([jnp.zeros_like(values[..., :1]), values[..., :-1]], axis=-1)


def coefficients(wind_u, wind_v, mixing):
    return (
        1.0 - 4.0 * mixing,
        mixing - 0.5 * wind_u,
        mixing + 0.5 * wind_u,
        mixing - 0.5 * wind_v,
        mixing + 0.5 * wind_v,
    )


def tangent_step(fields, coeffs, offset):
    extent = fields.shape[0]
    centre, eastward, westward, northward, southward = [
        coeff[offset + 1 : offset + extent - 1][:, None] for coeff in coeffs
    ]
    middle = fields[1:-1]
    return (
        centre * middle
        + eastward * fields[2:]
        + westward * fields[:-2]
        + northward * from_north(middle)
        + southward * from_south(middle)
    )


def adjoint_step(fields, coeffs, offset):
    extent = fields.shape[0]
    centre = coeffs[0][offset + 1 : offset + extent - 1][:, None]
    northward = coeffs[3][offset + 1 : offset + extent - 1][:, None]
    southward = coeffs[4][offset + 1 : offset + extent - 1][:, None]
    eastward = coeffs[1][offset : offset + extent][:, None]
    westward = coeffs[2][offset : offset + extent][:, None]
    middle = fields[1:-1]
    return (
        centre * middle
        + (eastward * fields)[:-2]
        + (westward * fields)[2:]
        + from_south(northward * middle)
        + from_north(southward * middle)
    )


def run_tangent(fields, coeffs, margin):
    for _ in range(STEPS // margin):
        grown = extended(fields, (("tiles", 0),), margin)
        for _ in range(margin):
            offset = (coeffs[0].shape[0] - grown.shape[0]) // 2
            grown = tangent_step(grown, coeffs, offset)
        fields = grown
    return fields


def run_adjoint(fields, coeffs, margin):
    for _ in range(STEPS // margin):
        grown = extended(fields, (("tiles", 0),), margin)
        for _ in range(margin):
            offset = (coeffs[0].shape[0] - grown.shape[0]) // 2
            grown = adjoint_step(grown, coeffs, offset)
        fields = grown
    return fields


def square_tables(extent):
    index = jnp.arange(extent, dtype=jnp.int32)
    phases = index[:, None] * index[None, :] % extent
    angles = phases.astype(jnp.float32) * (2.0 * math.pi / extent)
    return (jnp.cos(angles), jnp.sin(angles))


def contract(form, first, second):
    return jnp.einsum(form, first, second, precision=lax.Precision.HIGHEST)


def smooth_bands(bands, length_sq):
    count = bands.shape[0]
    inner = LON_DEV
    outer = count // inner
    columns = bands.reshape(outer, inner, -1)
    cos_outer, sin_outer = square_tables(outer)
    cos_inner, sin_inner = square_tables(inner)
    outer_index = jnp.arange(outer, dtype=jnp.int32)
    inner_index = jnp.arange(inner, dtype=jnp.int32)
    twist = (outer_index[:, None] * inner_index[None, :] % count).astype(jnp.float32) * (
        2.0 * math.pi / count
    )
    twist_cos = jnp.cos(twist)[:, :, None]
    twist_sin = jnp.sin(twist)[:, :, None]
    first_real = contract("ab,bqc->aqc", cos_outer, columns)
    first_imag = -contract("ab,bqc->aqc", sin_outer, columns)
    turned_real = first_real * twist_cos + first_imag * twist_sin
    turned_imag = first_imag * twist_cos - first_real * twist_sin
    modes_real = contract("aqc,kq->akc", turned_real, cos_inner) + contract(
        "aqc,kq->akc", turned_imag, sin_inner
    )
    modes_imag = contract("aqc,kq->akc", turned_imag, cos_inner) - contract(
        "aqc,kq->akc", turned_real, sin_inner
    )
    wave = (outer_index[:, None] + outer * inner_index[None, :]).astype(jnp.float32)
    basic = 1.0 - jnp.cos(wave * (2.0 * math.pi / count))
    damping = (1.0 + 2.0 * length_sq[None, None, :, None, :] * basic[:, :, None, None, None]) ** (
        -SWEEPS
    )
    damping = jnp.broadcast_to(damping, (outer, inner) + bands.shape[1:]).reshape(outer, inner, -1)
    modes_real = modes_real * damping
    modes_imag = modes_imag * damping
    back_real = contract("akc,kq->aqc", modes_real, cos_inner) - contract(
        "akc,kq->aqc", modes_imag, sin_inner
    )
    back_imag = contract("akc,kq->aqc", modes_imag, cos_inner) + contract(
        "akc,kq->aqc", modes_real, sin_inner
    )
    final_real = back_real * twist_cos - back_imag * twist_sin
    final_imag = back_imag * twist_cos + back_real * twist_sin
    smoothed = contract("ab,bqc->aqc", cos_outer, final_real) - contract(
        "ab,bqc->aqc", sin_outer, final_imag
    )
    return (smoothed / count).reshape(bands.shape)


def body(increment, dual_vector, wind_u, wind_v, land_sea, length_sq, spread):
    margin = 4
    mixing = 0.15 + 0.09 * land_sea.astype(jnp.float32)
    grown_u, grown_v, grown_mix = (
        extended(wind_u, (("tiles", 0),), margin),
        extended(wind_v, (("tiles", 0),), margin),
        extended(mixing, (("tiles", 0),), margin),
    )
    coeffs = coefficients(grown_u, grown_v, grown_mix[:, None, :])
    carried = passed_along(increment[:, -1:], "subwin", 1)
    previous = jnp.concatenate([carried, increment[:, :-1]], axis=1)
    later = passed_along(dual_vector[:, :1], "subwin", -1)
    following = jnp.concatenate([dual_vector[:, 1:], later], axis=1)
    weighted = dual_vector * spread[None, :, :, None]
    bands = lax.all_to_all(weighted, "tiles", split_axis=3, concat_axis=0, tiled=True)
    smoothed = smooth_bands(bands, length_sq)
    forward = run_tangent(previous, coeffs, margin)
    backward = run_adjoint(following, coeffs, margin)
    returned = lax.all_to_all(smoothed, "tiles", split_axis=0, concat_axis=3, tiled=True)
    covar = returned * spread[None, :, :, None]
    return (covar + increment - forward, dual_vector - backward)


SUB = 8
LANES = 128
VMEM_BYTES = 4 * 2**20


def dense_fits(mesh, shape):
    lons, wins, levels, lats = shape
    tiles = mesh.shape["tiles"]
    halves = levels // SUB
    return (
        levels % SUB == 0
        and wins * halves * lats == LANES
        and lons * halves * lats == LANES
        and LANES % levels == 0
        and lats % tiles == 0
        and lons * lats + wins * (lats // tiles) <= LANES
        and mesh.shape["subwin"] == 2
        and tiles % 2 == 0
        and tiles // 2 >= 4
        and STEPS <= 2 * lons
    )


def lane_index():
    return lax.broadcasted_iota(jnp.int32, (SUB, LANES), 1)


def picked(values, index):
    return jnp.take_along_axis(values, index, axis=1)


class Rows:
    def __init__(self, lons, tiles, main, peer, left, right, wide, narrow=None, *far):
        self.tiles = tiles
        self.even = lax.axis_index("tiles") % 2 == 0
        whole = {row - 1: row * SUB for row in range(2 * lons + 3)}
        held = {row - 1: row * SUB for row in range(lons + 1)}
        self.places = ({}, {})
        for odd, sign in enumerate((1, -1)):
            self.add(odd, 0, main, whole, 0, 0)
            self.add(odd, sign, peer, whole, 0, 0)
            self.add(odd, -2, left, whole, 0, 0)
            self.add(odd, 2, right, whole, 0, 0)
            self.add(odd, -sign, wide, whole, 0, 0)
            self.add(odd, 3 * sign, narrow, held, 0, 0)
            for k, ref in enumerate(far):
                self.add(odd, 2 * (k + 2), ref, held, 0, 0)
                self.add(odd, 2 * (k + 2) + sign, ref, held, lons, SUB // 2)

    def add(self, odd, offset, ref, rows, start, misc):
        for row, at in rows.items():
            at = misc if row < 0 else start * SUB + at
            self.places[odd][offset % self.tiles, row] = (ref, at)

    def __call__(self, offset, row):
        key = (offset % self.tiles, row)
        places = [self.places[odd][key] for odd in (0, 1)]
        if row < 0:
            values = [jnp.broadcast_to(ref[at : at + 1, :], (SUB, LANES)) for ref, at in places]
        else:
            values = [ref[at : at + SUB, :] for ref, at in places]
        if places[0][0] is places[1][0] and places[0][1] == places[1][1]:
            return values[0]
        return jnp.where(self.even, values[0], values[1])


def pack_kernel(*refs):
    arrays, main_ref, held, arrived = refs[:6], refs[6], refs[7:13], refs[13]
    copies = [
        pltpu.make_async_copy(source, target, arrived.at[k])
        for k, (source, target) in enumerate(zip(arrays, held))
    ]
    for copy in copies:
        copy.start()
    for copy in copies:
        copy.wait()
    inc_ref, dual_ref, u_ref, v_ref, land_ref, len_ref = held
    lons, wins, levels, lats = inc_ref.shape
    halves = levels // SUB
    own_lats = len_ref.shape[0]

    def put(row, slot, value):
        at = (row + 1) * SUB
        main_ref[at : at + SUB, slot * lats : (slot + 1) * lats] = value

    for i in range(lons):
        for half in range(halves):
            rows = slice(half * SUB, (half + 1) * SUB)
            for s in range(wins):
                put(i, s * halves + half, dual_ref[i, s, rows, :])
                put(lons + i, s * halves + half, inc_ref[i, s, rows, :])
            put(2 * lons, i * halves + half, 0.5 * u_ref[i, rows, :])
            put(2 * lons + 1, i * halves + half, 0.5 * v_ref[i, rows, :])
    main_ref[:SUB, :] = jnp.zeros((SUB, LANES), jnp.float32)
    for i in range(lons):
        mixing = 0.15 + 0.09 * land_ref[i : i + 1, :].astype(jnp.float32)
        main_ref[:SUB, i * lats : (i + 1) * lats] = jnp.broadcast_to(mixing, (SUB, lats))
    for j in range(own_lats):
        at = lons * lats + j * wins
        main_ref[:SUB, at : at + wins] = jnp.broadcast_to(
            len_ref[j : j + 1, :], (SUB, wins)
        )


def north(values):
    return pltpu.roll(values, LANES - 1, 1)


def south(values):
    return pltpu.roll(values, 1, 1)


def model_kernel(geometry, *refs):
    lons, wins, _, lats, tiles = geometry
    near, (forward_ref, backward_ref, edge_ref, coeff_ref) = refs[:-4], refs[-4:]
    group = LANES // wins
    rows = Rows(lons, tiles, *near)
    lane = lane_index()
    lat = lane % lats
    forward, backward = [], []
    for r in range(lons + 2 * STEPS):
        offset, i = (r - STEPS) // lons, (r - STEPS) % lons
        spot = i * group + lane % group
        wind_u = picked(rows(offset, 2 * lons), spot)
        wind_v = picked(rows(offset, 2 * lons + 1), spot)
        mixing = picked(rows(offset, -1), i * lats + lat)
        coeff_ref[r, 0] = 1.0 - 4.0 * mixing
        coeff_ref[r, 1] = mixing - wind_u
        coeff_ref[r, 2] = mixing + wind_u
        coeff_ref[r, 3] = jnp.where(lat == lats - 1, 0.0, mixing - wind_v)
        coeff_ref[r, 4] = jnp.where(lat == 0, 0.0, mixing + wind_v)
        forward.append(rows(offset, lons + i))
        backward.append(rows(offset, i))
    for step in range(STEPS):
        ahead, behind = [], []
        for p in range(1, len(forward) - 1):
            r = p + step
            middle = forward[p]
            ahead.append(
                coeff_ref[r, 0] * middle
                + coeff_ref[r, 1] * forward[p + 1]
                + coeff_ref[r, 2] * forward[p - 1]
                + coeff_ref[r, 3] * north(middle)
                + coeff_ref[r, 4] * south(middle)
            )
            middle = backward[p]
            behind.append(
                coeff_ref[r, 0] * middle
                + coeff_ref[r - 1, 1] * backward[p - 1]
                + coeff_ref[r + 1, 2] * backward[p + 1]
                + south(coeff_ref[r, 3] * middle)
                + north(coeff_ref[r, 4] * middle)
            )
        forward, backward = ahead, behind
    first = lax.axis_index("subwin") == 0
    for i in range(lons):
        at = slice(i * SUB, (i + 1) * SUB)
        forward_ref[at, :] = forward[i]
        backward_ref[at, :] = backward[i]
        edge_ref[at, :] = jnp.where(first, forward[i], backward[i])


def unpack(ref, i, value, wins, halves, lats):
    for s in range(wins):
        for half in range(halves):
            at = (s * halves + half) * lats
            ref[i, s, half * SUB : (half + 1) * SUB, :] = value[:, at : at + lats]


def filter_kernel(geometry, *refs):
    lons, wins, levels, lats, tiles = geometry
    group = LANES // wins
    own_lats = lats // tiles
    count = lons * tiles
    spread_ref, covar_ref = refs[-2:]
    rows = Rows(lons, tiles, *refs[:-2])
    lane = lane_index()
    tile = lax.axis_index("tiles")

    length = jnp.zeros((SUB, LANES), jnp.float32)
    index = lons * lats + wins * (lane % own_lats) + lane // group
    owner = lane % lats // own_lats
    for offset in range(tiles):
        here = picked(rows(offset, -1), index)
        length = jnp.where(owner == (tile + offset) % tiles, here, length)
    half = count // 2
    damped = []
    for wave in range(half + 1):
        basic = 1.0 - math.cos(2.0 * math.pi * wave / count)
        inverse = 1.0 / (1.0 + (2.0 * basic) * length)
        squared = inverse * inverse
        weight = (1.0 if wave in (0, half) else 2.0) / count
        damped.append(squared * (squared * weight))

    def waves(gap, start):
        total = None
        for wave in range(start, half + 1, 2):
            factor = math.cos(2.0 * math.pi * (wave * gap % count) / count)
            term = damped[wave] if factor == 1.0 else damped[wave] * factor
            total = term if total is None else total + term
        return total

    weights = [None] * (half + 1)
    for gap in range(half // 2 + 1):
        even, odd = waves(gap, 0), waves(gap, 1)
        weights[gap] = even + odd
        weights[half - gap] = even - odd if half % 2 == 0 else None
    for gap in range(half + 1):
        if weights[gap] is None:
            weights[gap] = waves(gap, 0) + waves(gap, 1)

    smooth = [None] * lons
    for offset in range(tiles):
        for j in range(lons):
            value = rows(offset, j)
            for i in range(lons):
                gap = (i - (offset * lons + j)) % count
                term = weights[min(gap, count - gap)] * value
                smooth[i] = term if smooth[i] is None else smooth[i] + term

    level = lax.broadcasted_iota(jnp.int32, (SUB, LANES), 0) + SUB * (lane % group // lats)
    scale = jnp.zeros((SUB, LANES), jnp.float32)
    for s in range(wins):
        row = jnp.concatenate(
            [jnp.broadcast_to(spread_ref[s : s + 1, :], (SUB, levels))] * (LANES // levels), axis=1
        )
        scale = jnp.where(lane // group == s, picked(row, level), scale)
    square = scale * scale
    for i in range(lons):
        covar_ref[i * SUB : (i + 1) * SUB, :] = square * smooth[i]


def finish_kernel(geometry, *refs):
    lons, wins, levels, lats, _ = geometry
    main, forward_ref, backward_ref, swapped_ref, covar_ref = refs[:5]
    outs, held, sent = refs[5:7], refs[7:9], refs[9]
    group = LANES // wins
    lane = lane_index()
    first = lax.axis_index("subwin") == 0
    copies = [pltpu.make_async_copy(held[k], outs[k], sent.at[k]) for k in (0, 1)]
    for i in range(lons):
        at = slice(i * SUB, (i + 1) * SUB)
        edge = jnp.where(first, swapped_ref[at, :], 0.0)
        behind = jnp.where(lane >= group, backward_ref[at, :], edge)
        value = main[(i + 1) * SUB : (i + 2) * SUB, :] - pltpu.roll(behind, LANES - group, 1)
        unpack(held[1], i, value, wins, levels // SUB, lats)
    copies[1].start()
    for i in range(lons):
        at = slice(i * SUB, (i + 1) * SUB)
        edge = jnp.where(first, 0.0, swapped_ref[at, :])
        ahead = jnp.where(lane < LANES - group, forward_ref[at, :], edge)
        increment = main[(lons + i + 1) * SUB : (lons + i + 2) * SUB, :]
        value = covar_ref[at, :] + increment - pltpu.roll(ahead, group, 1)
        unpack(held[0], i, value, wins, levels // SUB, lats)
    copies[0].start()
    for copy in copies:
        copy.wait()


def kernel_call(kernel, inputs, outputs, scratch=(), flops=0, space=pltpu.VMEM):
    vmem = pl.BlockSpec(memory_space=pltpu.VMEM)
    return pl.pallas_call(
        kernel,
        out_shape=outputs,
        in_specs=[vmem] * len(inputs),
        out_specs=(pl.BlockSpec(memory_space=space),) * len(outputs),
        scratch_shapes=list(scratch),
        compiler_params=pltpu.CompilerParams(vmem_limit_bytes=VMEM_BYTES),
        cost_estimate=pl.CostEstimate(flops=flops, bytes_accessed=2**18, transcendentals=0),
    )(*inputs)


def dense_body(increment, dual_vector, wind_u, wind_v, land_sea, length_sq, spread):
    lons, wins, levels, lats = increment.shape
    tiles = lax.axis_size("tiles")
    rings = tiles // 2
    geometry = (lons, wins, levels, lats, tiles)

    def rows(count):
        return jax.ShapeDtypeStruct((count * SUB, LANES), jnp.float32)

    full = jax.ShapeDtypeStruct(increment.shape, jnp.float32)
    arrays = (increment, dual_vector, wind_u, wind_v, land_sea, length_sq.T)
    main = pl.pallas_call(
        pack_kernel,
        out_shape=rows(2 * lons + 3),
        in_specs=[pl.BlockSpec(memory_space=pltpu.HBM)] * len(arrays),
        out_specs=pl.BlockSpec(memory_space=pltpu.VMEM),
        scratch_shapes=[pltpu.VMEM(x.shape, x.dtype) for x in arrays]
        + [pltpu.SemaphoreType.DMA((len(arrays),))],
        compiler_params=pltpu.CompilerParams(vmem_limit_bytes=VMEM_BYTES),
        name="pack",
    )(*[pltpu.with_memory_space_constraint(x, pltpu.HBM) for x in arrays])

    def moved(x, by):
        pairs = [(t, (t // 2 + by(t % 2)) % rings * 2 + t % 2) for t in range(tiles)]
        return lax.ppermute(x, "tiles", pairs)

    peer = lax.ppermute(main, "tiles", [(t, t ^ 1) for t in range(tiles)])
    row = lax.broadcasted_iota(jnp.int32, (SUB, LANES), 0)
    misc = jnp.where(row < SUB // 2, main[:SUB], peer[:SUB])
    held = (lons + 1) * SUB
    left = moved(main, lambda odd: 1)
    right = moved(main, lambda odd: -1)
    wide = lax.ppermute(
        main,
        "tiles",
        [(t, (t + 1 if t % 2 else t - 1) % tiles) for t in range(tiles)],
    )
    narrow = moved(peer[:held], lambda odd: 1 if odd else -1)
    short = jnp.concatenate([misc, main[SUB:held], peer[SUB:held]])
    far = [moved(short, lambda odd, d=d: -d) for d in range(2, rings - 1)]
    near = (main, peer, left, right, wide)
    span = lons + 2 * STEPS
    forward, backward, edge = kernel_call(
        functools.partial(model_kernel, geometry),
        near,
        (rows(lons),) * 3,
        [pltpu.VMEM((span, 5, SUB, LANES), jnp.float32)],
        flops=MODEL_FLOPS,
    )
    swapped = lax.ppermute(edge, "subwin", [(0, 1), (1, 0)])
    (covar,) = kernel_call(
        functools.partial(filter_kernel, geometry),
        (*near, narrow, *far, spread),
        (rows(lons),),
        flops=MODEL_FLOPS,
    )
    model_side, dual_side = kernel_call(
        functools.partial(finish_kernel, geometry),
        (main, forward, backward, swapped, covar),
        (full, full),
        [pltpu.VMEM(full.shape, full.dtype)] * 2 + [pltpu.SemaphoreType.DMA((2,))],
        flops=MODEL_FLOPS,
        space=pltpu.HBM,
    )
    return model_side, dual_side


def solution(mesh):
    placed = (
        P(("groups", "tiles"), "subwin", None, None),
        P(("groups", "tiles"), "subwin", None, None),
        P("tiles", None, None),
        P("tiles", None, None),
        P("tiles", None),
        P("subwin", "tiles"),
        P("subwin", None),
    )

    def local(*arrays):
        if dense_fits(mesh, arrays[0].shape):
            return dense_body(*arrays)
        return body(*arrays)

    return jax.shard_map(
        local,
        mesh=mesh,
        in_specs=placed,
        out_specs=(
            P(("groups", "tiles"), "subwin", None, None),
            P(("groups", "tiles"), "subwin", None, None),
        ),
        check_vma=False,
    )
```

```python
import functools
import math

import jax
import jax.numpy as jnp
from jax import lax
from jax.experimental import pallas as pl
from jax.experimental.pallas import tpu as pltpu
from jax.sharding import PartitionSpec as P


STEPS = 8
SWEEPS = 4
LON_DEV = 4
MODEL_FLOPS = 10**6


def extended(x, sides, width):
    for axis, dim in sides:
        devices, length = (lax.axis_size(axis), x.shape[dim])
        up = [(i, (i + 1) % devices) for i in range(devices)]
        down = [(j, i) for i, j in up]
        last = lax.slice_in_dim(x, length - width, length, axis=dim)
        leading = lax.slice_in_dim(x, 0, width, axis=dim)
        before = lax.ppermute(last, axis, up)
        after = lax.ppermute(leading, axis, down)
        x = jnp.concatenate([before, x, after], axis=dim)
    return x


def passed_along(x, axis, by):
    devices = lax.axis_size(axis)
    pairs = [(i, i + by) for i in range(devices) if 0 <= i + by < devices]
    return lax.ppermute(x, axis, pairs)


def from_north(values):
    return jnp.concatenate([values[..., 1:], jnp.zeros_like(values[..., :1])], axis=-1)


def from_south(values):
    return jnp.concatenate([jnp.zeros_like(values[..., :1]), values[..., :-1]], axis=-1)


def coefficients(wind_u, wind_v, mixing):
    return (
        1.0 - 4.0 * mixing,
        mixing - 0.5 * wind_u,
        mixing + 0.5 * wind_u,
        mixing - 0.5 * wind_v,
        mixing + 0.5 * wind_v,
    )


def tangent_step(fields, coeffs, offset):
    extent = fields.shape[0]
    centre, eastward, westward, northward, southward = [
        coeff[offset + 1 : offset + extent - 1][:, None] for coeff in coeffs
    ]
    middle = fields[1:-1]
    return (
        centre * middle
        + eastward * fields[2:]
        + westward * fields[:-2]
        + northward * from_north(middle)
        + southward * from_south(middle)
    )


def adjoint_step(fields, coeffs, offset):
    extent = fields.shape[0]
    centre = coeffs[0][offset + 1 : offset + extent - 1][:, None]
    northward = coeffs[3][offset + 1 : offset + extent - 1][:, None]
    southward = coeffs[4][offset + 1 : offset + extent - 1][:, None]
    eastward = coeffs[1][offset : offset + extent][:, None]
    westward = coeffs[2][offset : offset + extent][:, None]
    middle = fields[1:-1]
    return (
        centre * middle
        + (eastward * fields)[:-2]
        + (westward * fields)[2:]
        + from_south(northward * middle)
        + from_north(southward * middle)
    )


def run_tangent(fields, coeffs, margin):
    for _ in range(STEPS // margin):
        grown = extended(fields, (("tiles", 0),), margin)
        for _ in range(margin):
            offset = (coeffs[0].shape[0] - grown.shape[0]) // 2
            grown = tangent_step(grown, coeffs, offset)
        fields = grown
    return fields


def run_adjoint(fields, coeffs, margin):
    for _ in range(STEPS // margin):
        grown = extended(fields, (("tiles", 0),), margin)
        for _ in range(margin):
            offset = (coeffs[0].shape[0] - grown.shape[0]) // 2
            grown = adjoint_step(grown, coeffs, offset)
        fields = grown
    return fields


def square_tables(extent):
    index = jnp.arange(extent, dtype=jnp.int32)
    phases = index[:, None] * index[None, :] % extent
    angles = phases.astype(jnp.float32) * (2.0 * math.pi / extent)
    return (jnp.cos(angles), jnp.sin(angles))


def contract(form, first, second):
    return jnp.einsum(form, first, second, precision=lax.Precision.HIGHEST)


def smooth_bands(bands, length_sq):
    count = bands.shape[0]
    inner = LON_DEV
    outer = count // inner
    columns = bands.reshape(outer, inner, -1)
    cos_outer, sin_outer = square_tables(outer)
    cos_inner, sin_inner = square_tables(inner)
    outer_index = jnp.arange(outer, dtype=jnp.int32)
    inner_index = jnp.arange(inner, dtype=jnp.int32)
    twist = (outer_index[:, None] * inner_index[None, :] % count).astype(jnp.float32) * (
        2.0 * math.pi / count
    )
    twist_cos = jnp.cos(twist)[:, :, None]
    twist_sin = jnp.sin(twist)[:, :, None]
    first_real = contract("ab,bqc->aqc", cos_outer, columns)
    first_imag = -contract("ab,bqc->aqc", sin_outer, columns)
    turned_real = first_real * twist_cos + first_imag * twist_sin
    turned_imag = first_imag * twist_cos - first_real * twist_sin
    modes_real = contract("aqc,kq->akc", turned_real, cos_inner) + contract(
        "aqc,kq->akc", turned_imag, sin_inner
    )
    modes_imag = contract("aqc,kq->akc", turned_imag, cos_inner) - contract(
        "aqc,kq->akc", turned_real, sin_inner
    )
    wave = (outer_index[:, None] + outer * inner_index[None, :]).astype(jnp.float32)
    basic = 1.0 - jnp.cos(wave * (2.0 * math.pi / count))
    damping = (1.0 + 2.0 * length_sq[None, None, :, None, :] * basic[:, :, None, None, None]) ** (
        -SWEEPS
    )
    damping = jnp.broadcast_to(damping, (outer, inner) + bands.shape[1:]).reshape(outer, inner, -1)
    modes_real = modes_real * damping
    modes_imag = modes_imag * damping
    back_real = contract("akc,kq->aqc", modes_real, cos_inner) - contract(
        "akc,kq->aqc", modes_imag, sin_inner
    )
    back_imag = contract("akc,kq->aqc", modes_imag, cos_inner) + contract(
        "akc,kq->aqc", modes_real, sin_inner
    )
    final_real = back_real * twist_cos - back_imag * twist_sin
    final_imag = back_imag * twist_cos + back_real * twist_sin
    smoothed = contract("ab,bqc->aqc", cos_outer, final_real) - contract(
        "ab,bqc->aqc", sin_outer, final_imag
    )
    return (smoothed / count).reshape(bands.shape)


def body(increment, dual_vector, wind_u, wind_v, land_sea, length_sq, spread):
    margin = 4
    mixing = 0.15 + 0.09 * land_sea.astype(jnp.float32)
    grown_u, grown_v, grown_mix = (
        extended(wind_u, (("tiles", 0),), margin),
        extended(wind_v, (("tiles", 0),), margin),
        extended(mixing, (("tiles", 0),), margin),
    )
    coeffs = coefficients(grown_u, grown_v, grown_mix[:, None, :])
    carried = passed_along(increment[:, -1:], "subwin", 1)
    previous = jnp.concatenate([carried, increment[:, :-1]], axis=1)
    later = passed_along(dual_vector[:, :1], "subwin", -1)
    following = jnp.concatenate([dual_vector[:, 1:], later], axis=1)
    weighted = dual_vector * spread[None, :, :, None]
    bands = lax.all_to_all(weighted, "tiles", split_axis=3, concat_axis=0, tiled=True)
    smoothed = smooth_bands(bands, length_sq)
    forward = run_tangent(previous, coeffs, margin)
    backward = run_adjoint(following, coeffs, margin)
    returned = lax.all_to_all(smoothed, "tiles", split_axis=0, concat_axis=3, tiled=True)
    covar = returned * spread[None, :, :, None]
    return (covar + increment - forward, dual_vector - backward)


SUB = 8
LANES = 128
VMEM_BYTES = 4 * 2**20


def dense_fits(mesh, shape):
    lons, wins, levels, lats = shape
    tiles = mesh.shape["tiles"]
    halves = levels // SUB
    return (
        levels % SUB == 0
        and wins * halves * lats == LANES
        and lons * halves * lats == LANES
        and LANES % levels == 0
        and lats % tiles == 0
        and lons * lats + wins * (lats // tiles) <= LANES
        and mesh.shape["subwin"] == 2
        and tiles % 2 == 0
        and tiles // 2 >= 4
        and STEPS <= 2 * lons
    )


def lane_index():
    return lax.broadcasted_iota(jnp.int32, (SUB, LANES), 1)


def picked(values, index):
    return jnp.take_along_axis(values, index, axis=1)


class Rows:
    def __init__(self, lons, tiles, main, peer, left, right, wide, narrow=None, *far):
        self.tiles = tiles
        self.even = lax.axis_index("tiles") % 2 == 0
        whole = {row - 1: row * SUB for row in range(2 * lons + 3)}
        held = {row - 1: row * SUB for row in range(lons + 1)}
        self.places = ({}, {})
        for odd, sign in enumerate((1, -1)):
            self.add(odd, 0, main, whole, 0, 0)
            self.add(odd, sign, peer, whole, 0, 0)
            self.add(odd, -2, left, whole, 0, 0)
            self.add(odd, 2, right, whole, 0, 0)
            self.add(odd, -sign, wide, whole, 0, 0)
            self.add(odd, 3 * sign, narrow, held, 0, 0)
            for k, ref in enumerate(far):
                self.add(odd, 2 * (k + 2), ref, held, 0, 0)
                self.add(odd, 2 * (k + 2) + sign, ref, held, lons, SUB // 2)

    def add(self, odd, offset, ref, rows, start, misc):
        for row, at in rows.items():
            at = misc if row < 0 else start * SUB + at
            self.places[odd][offset % self.tiles, row] = (ref, at)

    def __call__(self, offset, row):
        key = (offset % self.tiles, row)
        places = [self.places[odd][key] for odd in (0, 1)]
        if row < 0:
            values = [jnp.broadcast_to(ref[at : at + 1, :], (SUB, LANES)) for ref, at in places]
        else:
            values = [ref[at : at + SUB, :] for ref, at in places]
        if places[0][0] is places[1][0] and places[0][1] == places[1][1]:
            return values[0]
        return jnp.where(self.even, values[0], values[1])


def pack_kernel(*refs):
    arrays, main_ref, held, arrived = refs[:6], refs[6], refs[7:13], refs[13]
    copies = [
        pltpu.make_async_copy(source, target, arrived.at[k])
        for k, (source, target) in enumerate(zip(arrays, held))
    ]
    for copy in copies:
        copy.start()
    for copy in copies:
        copy.wait()
    inc_ref, dual_ref, u_ref, v_ref, land_ref, len_ref = held
    lons, wins, levels, lats = inc_ref.shape
    halves = levels // SUB
    own_lats = len_ref.shape[0]

    def put(row, slot, value):
        at = (row + 1) * SUB
        main_ref[at : at + SUB, slot * lats : (slot + 1) * lats] = value

    for i in range(lons):
        for half in range(halves):
            rows = slice(half * SUB, (half + 1) * SUB)
            for s in range(wins):
                put(i, s * halves + half, dual_ref[i, s, rows, :])
                put(lons + i, s * halves + half, inc_ref[i, s, rows, :])
            put(2 * lons, i * halves + half, 0.5 * u_ref[i, rows, :])
            put(2 * lons + 1, i * halves + half, 0.5 * v_ref[i, rows, :])
    main_ref[:SUB, :] = jnp.zeros((SUB, LANES), jnp.float32)
    for i in range(lons):
        mixing = 0.15 + 0.09 * land_ref[i : i + 1, :].astype(jnp.float32)
        main_ref[:SUB, i * lats : (i + 1) * lats] = jnp.broadcast_to(mixing, (SUB, lats))
    for j in range(own_lats):
        at = lons * lats + j * wins
        main_ref[:SUB, at : at + wins] = jnp.broadcast_to(
            len_ref[j : j + 1, :], (SUB, wins)
        )


def north(values):
    return pltpu.roll(values, LANES - 1, 1)


def south(values):
    return pltpu.roll(values, 1, 1)


def model_kernel(geometry, *refs):
    lons, wins, _, lats, tiles = geometry
    near, (forward_ref, backward_ref, edge_ref, coeff_ref) = refs[:-4], refs[-4:]
    group = LANES // wins
    rows = Rows(lons, tiles, *near)
    lane = lane_index()
    lat = lane % lats
    forward, backward = [], []
    for r in range(lons + 2 * STEPS):
        offset, i = (r - STEPS) // lons, (r - STEPS) % lons
        spot = i * group + lane % group
        wind_u = picked(rows(offset, 2 * lons), spot)
        wind_v = picked(rows(offset, 2 * lons + 1), spot)
        mixing = picked(rows(offset, -1), i * lats + lat)
        coeff_ref[r, 0] = 1.0 - 4.0 * mixing
        coeff_ref[r, 1] = mixing - wind_u
        coeff_ref[r, 2] = mixing + wind_u
        coeff_ref[r, 3] = jnp.where(lat == lats - 1, 0.0, mixing - wind_v)
        coeff_ref[r, 4] = jnp.where(lat == 0, 0.0, mixing + wind_v)
        forward.append(rows(offset, lons + i))
        backward.append(rows(offset, i))
    for step in range(STEPS):
        ahead, behind = [], []
        for p in range(1, len(forward) - 1):
            r = p + step
            middle = forward[p]
            ahead.append(
                coeff_ref[r, 0] * middle
                + coeff_ref[r, 1] * forward[p + 1]
                + coeff_ref[r, 2] * forward[p - 1]
                + coeff_ref[r, 3] * north(middle)
                + coeff_ref[r, 4] * south(middle)
            )
            middle = backward[p]
            behind.append(
                coeff_ref[r, 0] * middle
                + coeff_ref[r - 1, 1] * backward[p - 1]
                + coeff_ref[r + 1, 2] * backward[p + 1]
                + south(coeff_ref[r, 3] * middle)
                + north(coeff_ref[r, 4] * middle)
            )
        forward, backward = ahead, behind
    first = lax.axis_index("subwin") == 0
    for i in range(lons):
        at = slice(i * SUB, (i + 1) * SUB)
        forward_ref[at, :] = forward[i]
        backward_ref[at, :] = backward[i]
        edge_ref[at, :] = jnp.where(first, forward[i], backward[i])


def unpack(ref, i, value, wins, halves, lats):
    for s in range(wins):
        for half in range(halves):
            at = (s * halves + half) * lats
            ref[i, s, half * SUB : (half + 1) * SUB, :] = value[:, at : at + lats]


def filtered(geometry, spread_ref, *refs):
    lons, wins, levels, lats, tiles = geometry
    group = LANES // wins
    own_lats = lats // tiles
    count = lons * tiles
    rows = Rows(lons, tiles, *refs)
    lane = lane_index()
    tile = lax.axis_index("tiles")

    length = jnp.zeros((SUB, LANES), jnp.float32)
    index = lons * lats + wins * (lane % own_lats) + lane // group
    owner = lane % lats // own_lats
    for offset in range(tiles):
        here = picked(rows(offset, -1), index)
        length = jnp.where(owner == (tile + offset) % tiles, here, length)
    half = count // 2
    damped = []
    for wave in range(half + 1):
        basic = 1.0 - math.cos(2.0 * math.pi * wave / count)
        inverse = 1.0 / (1.0 + (2.0 * basic) * length)
        squared = inverse * inverse
        weight = (1.0 if wave in (0, half) else 2.0) / count
        damped.append(squared * (squared * weight))

    def waves(gap, start):
        total = None
        for wave in range(start, half + 1, 2):
            factor = math.cos(2.0 * math.pi * (wave * gap % count) / count)
            term = damped[wave] if factor == 1.0 else damped[wave] * factor
            total = term if total is None else total + term
        return total

    weights = [None] * (half + 1)
    for gap in range(half // 2 + 1):
        even, odd = waves(gap, 0), waves(gap, 1)
        weights[gap] = even + odd
        weights[half - gap] = even - odd if half % 2 == 0 else None
    for gap in range(half + 1):
        if weights[gap] is None:
            weights[gap] = waves(gap, 0) + waves(gap, 1)

    smooth = [None] * lons
    for offset in range(tiles):
        for j in range(lons):
            value = rows(offset, j)
            for i in range(lons):
                gap = (i - (offset * lons + j)) % count
                term = weights[min(gap, count - gap)] * value
                smooth[i] = term if smooth[i] is None else smooth[i] + term

    level = lax.broadcasted_iota(jnp.int32, (SUB, LANES), 0) + SUB * (lane % group // lats)
    scale = jnp.zeros((SUB, LANES), jnp.float32)
    for s in range(wins):
        row = jnp.concatenate(
            [jnp.broadcast_to(spread_ref[s : s + 1, :], (SUB, levels))] * (LANES // levels), axis=1
        )
        scale = jnp.where(lane // group == s, picked(row, level), scale)
    square = scale * scale
    for i in range(lons):
        smooth[i] = square * smooth[i]
    return smooth


def finish_kernel(geometry, *refs):
    lons, wins, levels, lats, _ = geometry
    main, forward_ref, backward_ref, swapped_ref, spread_ref = refs[0], *refs[-9:-5]
    outs, held, sent = refs[-5:-3], refs[-3:-1], refs[-1]
    group = LANES // wins
    lane = lane_index()
    first = lax.axis_index("subwin") == 0
    copies = [pltpu.make_async_copy(held[k], outs[k], sent.at[k]) for k in (0, 1)]
    for i in range(lons):
        at = slice(i * SUB, (i + 1) * SUB)
        edge = jnp.where(first, swapped_ref[at, :], 0.0)
        behind = jnp.where(lane >= group, backward_ref[at, :], edge)
        value = main[(i + 1) * SUB : (i + 2) * SUB, :] - pltpu.roll(behind, LANES - group, 1)
        unpack(held[1], i, value, wins, levels // SUB, lats)
    copies[1].start()
    covar = filtered(geometry, spread_ref, *refs[:-9])
    for i in range(lons):
        at = slice(i * SUB, (i + 1) * SUB)
        edge = jnp.where(first, 0.0, swapped_ref[at, :])
        ahead = jnp.where(lane < LANES - group, forward_ref[at, :], edge)
        increment = main[(lons + i + 1) * SUB : (lons + i + 2) * SUB, :]
        value = covar[i] + increment - pltpu.roll(ahead, group, 1)
        unpack(held[0], i, value, wins, levels // SUB, lats)
    copies[0].start()
    for copy in copies:
        copy.wait()


def kernel_call(kernel, inputs, outputs, scratch=(), flops=0, space=pltpu.VMEM):
    vmem = pl.BlockSpec(memory_space=pltpu.VMEM)
    return pl.pallas_call(
        kernel,
        out_shape=outputs,
        in_specs=[vmem] * len(inputs),
        out_specs=(pl.BlockSpec(memory_space=space),) * len(outputs),
        scratch_shapes=list(scratch),
        compiler_params=pltpu.CompilerParams(vmem_limit_bytes=VMEM_BYTES),
        cost_estimate=pl.CostEstimate(flops=flops, bytes_accessed=2**18, transcendentals=0),
    )(*inputs)


def dense_body(increment, dual_vector, wind_u, wind_v, land_sea, length_sq, spread):
    lons, wins, levels, lats = increment.shape
    tiles = lax.axis_size("tiles")
    rings = tiles // 2
    geometry = (lons, wins, levels, lats, tiles)

    def rows(count):
        return jax.ShapeDtypeStruct((count * SUB, LANES), jnp.float32)

    full = jax.ShapeDtypeStruct(increment.shape, jnp.float32)
    arrays = (increment, dual_vector, wind_u, wind_v, land_sea, length_sq.T)
    main = pl.pallas_call(
        pack_kernel,
        out_shape=rows(2 * lons + 3),
        in_specs=[pl.BlockSpec(memory_space=pltpu.HBM)] * len(arrays),
        out_specs=pl.BlockSpec(memory_space=pltpu.VMEM),
        scratch_shapes=[pltpu.VMEM(x.shape, x.dtype) for x in arrays]
        + [pltpu.SemaphoreType.DMA((len(arrays),))],
        compiler_params=pltpu.CompilerParams(vmem_limit_bytes=VMEM_BYTES),
        name="pack",
    )(*[pltpu.with_memory_space_constraint(x, pltpu.HBM) for x in arrays])

    def moved(x, by):
        pairs = [(t, (t // 2 + by(t % 2)) % rings * 2 + t % 2) for t in range(tiles)]
        return lax.ppermute(x, "tiles", pairs)

    peer = lax.ppermute(main, "tiles", [(t, t ^ 1) for t in range(tiles)])
    row = lax.broadcasted_iota(jnp.int32, (SUB, LANES), 0)
    misc = jnp.where(row < SUB // 2, main[:SUB], peer[:SUB])
    held = (lons + 1) * SUB
    left = moved(main, lambda odd: 1)
    right = moved(main, lambda odd: -1)
    wide = lax.ppermute(
        main,
        "tiles",
        [(t, (t + 1 if t % 2 else t - 1) % tiles) for t in range(tiles)],
    )
    narrow = moved(peer[:held], lambda odd: 1 if odd else -1)
    short = jnp.concatenate([misc, main[SUB:held], peer[SUB:held]])
    far = [moved(short, lambda odd, d=d: -d) for d in range(2, rings - 1)]
    near = (main, peer, left, right, wide)
    span = lons + 2 * STEPS
    forward, backward, edge = kernel_call(
        functools.partial(model_kernel, geometry),
        near,
        (rows(lons),) * 3,
        [pltpu.VMEM((span, 5, SUB, LANES), jnp.float32)],
        flops=MODEL_FLOPS,
    )
    swapped = lax.ppermute(edge, "subwin", [(0, 1), (1, 0)])
    model_side, dual_side = kernel_call(
        functools.partial(finish_kernel, geometry),
        (*near, narrow, *far, forward, backward, swapped, spread),
        (full, full),
        [pltpu.VMEM(full.shape, full.dtype)] * 2 + [pltpu.SemaphoreType.DMA((2,))],
        flops=MODEL_FLOPS,
        space=pltpu.HBM,
    )
    return model_side, dual_side


def solution(mesh):
    placed = (
        P(("groups", "tiles"), "subwin", None, None),
        P(("groups", "tiles"), "subwin", None, None),
        P("tiles", None, None),
        P("tiles", None, None),
        P("tiles", None),
        P("subwin", "tiles"),
        P("subwin", None),
    )

    def local(*arrays):
        if dense_fits(mesh, arrays[0].shape):
            return dense_body(*arrays)
        return body(*arrays)

    return jax.shard_map(
        local,
        mesh=mesh,
        in_specs=placed,
        out_specs=(
            P(("groups", "tiles"), "subwin", None, None),
            P(("groups", "tiles"), "subwin", None, None),
        ),
        check_vma=False,
    )
```
